512 devices in a mesh: groups: 2 (over y), rows: 32 (over z), cols: 4 (over x), sub: 2 (over core).
Axes of the slice: x: 4, y: 2, z: 32, core: 2. Of those that a mesh axis runs over, the one named last changes fastest.
The devices are a block of a 4x8x32 slice.
Arguments:
- returns: float32 [8, 512, 8192], P('groups', 'rows', ('cols', 'sub')), parts along dimension 0, may hold values from -6 to 6
- starts: int32 [8, 8192], P('groups', ('cols', 'sub')), parts along dimension 0, may hold values from 0 to 256
- start_block: float32 [8, 32, 8192], P('groups', None, ('cols', 'sub')), parts along dimension 0, may hold values from -6 to 6
Outputs:
- loadings: float32 [8, 32, 8192], P('groups', None, ('cols', 'sub')), parts along dimension 0
The draws below stay inside these ranges and needn't reach their ends.
There are 2 independent parts, one for each index of `groups`. The reference program is written for one: setup_inputs(seed, part) draws one part's arguments, and reference() takes and returns one part's arrays. A program takes and returns all parts, laid end to end along the dimension named above; each array names one. Nothing has to cross between parts.
Inputs may be any that keep to these rules, and one draw needn't show every extreme that they name: `starts`: days before an asset's start day hold returns that do not count.
All inputs are finite; a program needn't handle non-finite values.
Results may differ from the reference program's by a relative error of at most 0.0078.
Values may be sent and summed in bfloat16 or wider, within the bound.
No kernel may reach another device: no remote copies, remote signals or barrier semaphores. Data moves between devices by JAX's collectives and lax.ppermute only.
A program may use at most 64 MiB of HBM per device.

```python
import jax
import jax.numpy as jnp
from jax import lax

ASSETS = 8192
K = 32
ITERS = 3
NWIN = 4
TIME = 512


def place_ends(array, rng, low, top_value):
    dims = array.shape
    index_at = [jax.random.randint(jax.random.fold_in(rng, axis), (), 0, dims[axis]) for axis in range(len(dims))]
    array = array.at[tuple(index_at)].set(low)
    longest = dims.index(max(dims))
    index_at[longest] = (index_at[longest] + 1) % dims[longest]
    return array.at[tuple(index_at)].set(top_value)


def block_scale(own_key, extent, cuts, least, high):
    def one(dim, parts):
        heights = jax.random.uniform(jax.random.fold_in(jax.random.fold_in(own_key, 6), dim), (parts,), jnp.float32, least / len(cuts), high / len(cuts))
        return jnp.repeat(jnp.exp(heights), extent[dim] // parts).reshape((-1,) + (1,) * (len(extent) - dim - 1))

    gain = one(*cuts[0])
    for cut in cuts[1:]:
        gain = gain * one(*cut)
    return gain


def noise(own_key, shape, width, limit, shards=(), kind=jnp.bfloat16):
    level = block_scale(own_key, shape, shards, -0.22, 0.18) if shards else 1.0
    array = jax.random.normal(own_key, shape, jnp.float32) * width * level
    return jnp.minimum(jnp.maximum(array, -limit), limit).astype(kind)


def setup_inputs(seed: int = 0, part: int = 0) -> dict:
    key_list = jax.random.split(jax.random.key(seed), 4)
    own_keys = jax.random.split(jax.random.fold_in(key_list[3], part), 4)
    returns = noise(own_keys[0], (NWIN, TIME, ASSETS), 1.0, 6.0, ((1, 32), (2, 8)), jnp.float32)
    starts = place_ends(jax.random.randint(own_keys[1], (NWIN, ASSETS), 0, TIME // 2 + 1), jax.random.fold_in(own_keys[1], 1), 0, (TIME // 2 + 1) - 1).astype(jnp.int32)
    start_block = noise(own_keys[2], (NWIN, K, ASSETS), 1.0, 6.0, ((2, 8),), jnp.float32)
    return dict(returns=returns, starts=starts, start_block=start_block)


def standardize(returns, starts):
    days = jnp.arange(TIME, dtype=jnp.int32)
    live = (days[None, :, None] >= starts[:, None, :]).astype(jnp.float32)
    counts = (TIME - starts).astype(jnp.float32)
    mean = lax.optimization_barrier(jnp.sum(live * returns, axis=1)) / counts
    centered = live * (returns - mean[:, None, :])
    squares = lax.optimization_barrier(jnp.sum(centered * centered, axis=1))
    return (centered * lax.rsqrt(squares + 1.0)[:, None, :]).astype(jnp.bfloat16)

def one_window(pair):
    scaled, factors = pair
    widened = scaled.astype(jnp.float32)
    for step in range(ITERS):
        rounded = factors.astype(jnp.bfloat16)
        proj = jnp.dot(rounded.astype(jnp.float32), scaled.T.astype(jnp.float32), preferred_element_type=jnp.float32)
        image = jnp.dot(proj, widened, precision=lax.Precision.HIGHEST)
        gram = jnp.dot(image, image.T, precision=lax.Precision.HIGHEST) / ASSETS
        lower = jnp.linalg.cholesky(gram)
        factors = jax.scipy.linalg.solve_triangular(lower, image, lower=True)
    return factors

def reference(returns, starts, start_block):
    scaled = standardize(returns, starts)
    return lax.map(one_window, (scaled, start_block))
```

```python
import functools

import jax
import jax.numpy as jnp
from jax import lax
from jax.experimental import pallas as pl
from jax.experimental.pallas import tpu as pltpu
from jax.sharding import Mesh
from jax.sharding import PartitionSpec as P

ITERS = 3
LANES = 128
EXTRA = 8
F32 = jnp.float32
BF16 = jnp.bfloat16
HIGHEST = lax.Precision.HIGHEST
VMEM = pl.BlockSpec(memory_space=pltpu.VMEM)
SMEM = pl.BlockSpec(memory_space=pltpu.SMEM)


def dot(a, b, dims, precision=HIGHEST):
    return lax.dot_general(a, b, (dims, ((), ())), precision=precision, preferred_element_type=F32)


def pack_kernel(where_ref, returns_ref, starts_ref, out_ref):
    windows, days, width = returns_ref.shape
    parts = width // LANES
    day = lax.broadcasted_iota(jnp.int32, (days, width), 0) + where_ref[0] * days
    row = lax.broadcasted_iota(jnp.int32, (EXTRA, width), 0)
    for w in range(windows):
        live = day >= starts_ref[w : w + 1, :]
        kept = jnp.where(live, returns_ref[w], 0.0)
        number = jnp.sum(live.astype(F32), axis=0, keepdims=True)
        shift = jnp.sum(kept, axis=0, keepdims=True) / jnp.maximum(number, 1.0)
        high = shift.astype(BF16).astype(F32)
        middle = (shift - high).astype(BF16).astype(F32)
        low = (shift - high - middle).astype(BF16).astype(F32)
        shift = high + middle + low
        rest = jnp.where(live, kept - shift, 0.0).astype(BF16)
        carried = jnp.where(row == 0, high, jnp.where(row == 1, middle, jnp.where(row == 2, low, 0.0))).astype(BF16)
        for j in range(parts):
            at = slice(j * LANES, (j + 1) * LANES)
            out_ref[w * parts + j, 0:days, :] = rest[:, at]
            out_ref[w * parts + j, days : days + EXTRA, :] = carried[:, at]


def tiles_of(days):
    blocks = days // LANES
    return [(a, b) for a in range(blocks) for b in range(a, blocks)]


def gram_kernel(where_ref, got_ref, starts_ref, block_ref, scaled_ref, out_ref):
    sources, rows, _ = got_ref.shape
    days = rows - EXTRA
    total = sources * days
    w = where_ref[0]
    starts = starts_ref[pl.ds(w, 1), :]
    got = got_ref[...].astype(F32)
    shift = jnp.sum(got[:, days:, :], axis=1, keepdims=True)
    values = (got[:, :days, :] + shift).reshape(total, LANES)
    live = lax.broadcasted_iota(jnp.int32, (total, LANES), 0) >= starts
    counts = (total - starts).astype(F32)
    mean = jnp.sum(jnp.where(live, values, 0.0), axis=0, keepdims=True) / counts
    centered = jnp.where(live, values - mean, 0.0)
    squares = jnp.sum(centered * centered, axis=0, keepdims=True)
    scaled = centered * lax.rsqrt(squares + 1.0)
    scaled_ref[...] = scaled
    blocks = total // LANES
    at = 0
    for a in range(blocks):
        strip = dot(scaled[a * LANES : (a + 1) * LANES], scaled[a * LANES :], ((1,), (1,)))
        for b in range(a, blocks):
            out_ref[at : at + LANES, :] = strip[:, (b - a) * LANES : (b - a + 1) * LANES]
            at += LANES
    rounded = block_ref[0].astype(BF16).astype(F32)
    proj = dot(rounded, scaled, ((1,), (1,)))
    factors = proj.shape[0]
    for b in range(blocks):
        out_ref[at : at + factors, :] = proj[:, b * LANES : (b + 1) * LANES]
        at += factors
    if at < out_ref.shape[0]:
        out_ref[at:, :] = jnp.zeros((out_ref.shape[0] - at, LANES), F32)


def inverse_lower(gram):
    k = gram.shape[0]
    row = lax.broadcasted_iota(jnp.int32, (k, LANES), 0)
    lane = lax.broadcasted_iota(jnp.int32, (k, LANES), 1)
    both = jnp.concatenate([gram, jnp.zeros((k, LANES - k), F32)], axis=1)
    both = jnp.where(lane == row + k, 1.0, both)
    for i in range(k - 1):
        column = jnp.where(row > i, both[:, i : i + 1], 0.0)
        line = both[i : i + 1, :]
        both = both - column * (line / both[i : i + 1, i : i + 1])
    pivots = jnp.sum(jnp.where(lane == row, both, 0.0), axis=1, keepdims=True)
    return (both * lax.rsqrt(pivots))[:, k : 2 * k]


def iterate_kernel(assets, got_ref, scaled_ref, out_ref, gram_ref):
    total = scaled_ref.shape[0]
    factors = out_ref.shape[1]
    blocks = total // LANES
    at = 0
    for a, b in tiles_of(total):
        tile = got_ref[at : at + LANES, :]
        gram_ref[a * LANES : (a + 1) * LANES, b * LANES : (b + 1) * LANES] = tile
        if a != b:
            gram_ref[b * LANES : (b + 1) * LANES, a * LANES : (a + 1) * LANES] = tile.T
        at += LANES
    proj = jnp.concatenate([got_ref[at + b * factors : at + (b + 1) * factors, :] for b in range(blocks)], axis=1)
    for step in range(ITERS):
        moved = dot(proj, gram_ref[...], ((1,), (0,)))
        gram = dot(moved, proj, ((1,), (1,))) * (1.0 / assets)
        inverse = inverse_lower(gram)
        proj = dot(inverse, moved if step < ITERS - 1 else proj, ((1,), (0,)))
    loadings = dot(proj, scaled_ref[...], ((1,), (0,))).astype(BF16)
    out_ref[...] = jnp.broadcast_to(loadings[None], out_ref.shape)


def unpack_kernel(got_ref, out_ref):
    windows, _, width = out_ref.shape
    parts = width // LANES
    for w in range(windows):
        for j in range(parts):
            out_ref[w, :, j * LANES : (j + 1) * LANES] = got_ref[w * parts + j].astype(F32)


def on_device(returns, starts, start_block):
    windows, days, width = returns.shape
    factors = start_block.shape[1]
    parts = width // LANES
    rows = windows * parts
    sides = lax.axis_size(("cols", "sub"))
    total = days * rows
    assets = width * sides
    w, j = lax.axis_index("window"), lax.axis_index("part")
    row = w * parts + j

    packed = pl.pallas_call(
        pack_kernel,
        out_shape=jax.ShapeDtypeStruct((rows, days + EXTRA, LANES), BF16),
        in_specs=[SMEM, VMEM, VMEM],
        out_specs=VMEM,
        name="pack",
    )(row[None], returns, starts)
    got = lax.all_to_all(packed, ("window", "part"), 0, 0, tiled=True)

    filled = len(tiles_of(total)) * LANES + factors * total // LANES
    unit = 8 * sides * parts
    height = (filled + unit - 1) // unit * unit
    scaled, partial = pl.pallas_call(
        gram_kernel,
        out_shape=(
            jax.ShapeDtypeStruct((total, LANES), F32),
            jax.ShapeDtypeStruct((height, LANES), F32),
        ),
        grid_spec=pltpu.PrefetchScalarGridSpec(
            num_scalar_prefetch=1,
            grid=(1,),
            in_specs=[
                pl.BlockSpec((rows, days + EXTRA, LANES), lambda g, s: (0, 0, 0)),
                pl.BlockSpec((windows, LANES), lambda g, s: (0, s[1])),
                pl.BlockSpec((1, factors, LANES), lambda g, s: (s[0], 0, s[1])),
            ],
            out_specs=(
                pl.BlockSpec((total, LANES), lambda g, s: (0, 0)),
                pl.BlockSpec((height, LANES), lambda g, s: (0, 0)),
            ),
        ),
        name="gram",
    )(jnp.stack([w, j]), got, starts, start_block)

    own = lax.all_to_all(partial.reshape(sides, height // sides, LANES), ("cols", "sub"), 0, 0, tiled=True)
    own = own.sum(axis=0).reshape(parts, height // sides // parts, LANES)
    own = lax.all_to_all(own, "part", 0, 0, tiled=True).sum(axis=0)
    own = lax.all_to_all(jnp.broadcast_to(own[None], (parts, *own.shape)), "part", 0, 0, tiled=True)
    whole = lax.all_gather(own.reshape(height // sides, LANES), ("cols", "sub"), tiled=True)

    sent = pl.pallas_call(
        functools.partial(iterate_kernel, assets),
        out_shape=jax.ShapeDtypeStruct((rows, factors, LANES), BF16),
        in_specs=[VMEM, VMEM],
        out_specs=VMEM,
        scratch_shapes=[pltpu.VMEM((total, total), F32)],
        name="iterate",
    )(whole, scaled)
    got = lax.all_to_all(sent, ("window", "part"), 0, 0, tiled=True)
    return pl.pallas_call(
        unpack_kernel,
        out_shape=jax.ShapeDtypeStruct((windows, factors, width), F32),
        in_specs=[VMEM],
        out_specs=VMEM,
        name="unpack",
    )(got)


def solution(mesh):
    groups, rows, cols, sub = (mesh.shape[name] for name in ("groups", "rows", "cols", "sub"))

    def whole(returns, starts, start_block):
        windows = returns.shape[0] // groups
        split = Mesh(
            mesh.devices.reshape(groups, windows, rows // windows, cols, sub),
            ("groups", "window", "part", "cols", "sub"),
        )
        placed = (
            P("groups", ("window", "part"), ("cols", "sub")),
            P("groups", ("cols", "sub")),
            P("groups", None, ("cols", "sub")),
        )
        return jax.shard_map(
            on_device,
            mesh=split,
            in_specs=placed,
            out_specs=P("groups", None, ("cols", "sub")),
            check_vma=False,
        )(returns, starts, start_block)

    return whole
```

```python
import functools

import jax
import jax.numpy as jnp
from jax import lax
from jax.experimental import pallas as pl
from jax.experimental.pallas import tpu as pltpu
from jax.sharding import Mesh
from jax.sharding import PartitionSpec as P

ITERS = 3
LANES = 128
EXTRA = 8
F32 = jnp.float32
BF16 = jnp.bfloat16
HIGHEST = lax.Precision.HIGHEST
VMEM = pl.BlockSpec(memory_space=pltpu.VMEM)
SMEM = pl.BlockSpec(memory_space=pltpu.SMEM)
PARAMS = pltpu.CompilerParams(vmem_limit_bytes=16 << 20)


def dot(a, b, dims, precision=HIGHEST):
    return lax.dot_general(a, b, (dims, ((), ())), precision=precision, preferred_element_type=F32)


def split(a):
    high = a.astype(BF16)
    return high, (a - high.astype(F32)).astype(BF16)


def dot3(a, b, dims):
    (ah, al), (bh, bl) = split(a), split(b)
    return dot(ah, bh, dims, None) + (dot(al, bh, dims, None) + dot(ah, bl, dims, None))


def pack_kernel(where_ref, returns_ref, starts_ref, out_ref):
    windows, days, width = returns_ref.shape
    parts = width // LANES
    day = lax.broadcasted_iota(jnp.int32, (days, width), 0) + where_ref[0] * days
    row = lax.broadcasted_iota(jnp.int32, (EXTRA, width), 0)
    for w in range(windows):
        live = day >= starts_ref[w : w + 1, :]
        kept = jnp.where(live, returns_ref[w], 0.0)
        number = jnp.sum(live.astype(F32), axis=0, keepdims=True)
        shift = jnp.sum(kept, axis=0, keepdims=True) / jnp.maximum(number, 1.0)
        high = shift.astype(BF16).astype(F32)
        middle = (shift - high).astype(BF16).astype(F32)
        low = (shift - high - middle).astype(BF16).astype(F32)
        shift = high + middle + low
        rest = jnp.where(live, kept - shift, 0.0).astype(BF16)
        carried = jnp.where(row == 0, high, jnp.where(row == 1, middle, jnp.where(row == 2, low, 0.0))).astype(BF16)
        for j in range(parts):
            at = slice(j * LANES, (j + 1) * LANES)
            out_ref[w * parts + j, 0:days, :] = rest[:, at]
            out_ref[w * parts + j, days : days + EXTRA, :] = carried[:, at]


def tiles_of(days):
    blocks = days // LANES
    return [(a, b) for a in range(blocks) for b in range(a, blocks)]


def gram_kernel(got_ref, starts_ref, block_ref, scaled_ref, out_ref):
    sources, rows, _ = got_ref.shape
    days = rows - EXTRA
    total = sources * days
    starts = starts_ref[...]
    got = got_ref[...].astype(F32)
    shift = jnp.sum(got[:, days:, :], axis=1, keepdims=True)
    values = (got[:, :days, :] + shift).reshape(total, LANES)
    live = lax.broadcasted_iota(jnp.int32, (total, LANES), 0) >= starts
    counts = (total - starts).astype(F32)
    mean = jnp.sum(jnp.where(live, values, 0.0), axis=0, keepdims=True) / counts
    centered = jnp.where(live, values - mean, 0.0)
    squares = jnp.sum(centered * centered, axis=0, keepdims=True)
    scaled = centered * lax.rsqrt(squares + 1.0)
    scaled_ref[...] = scaled
    high, low = split(scaled)
    blocks = total // LANES
    across = ((1,), (1,))
    at = 0
    for a in range(blocks):
        here, on = slice(a * LANES, (a + 1) * LANES), slice(a * LANES, total)
        strip = dot(high[here], high[on], across, None)
        strip += dot(low[here], high[on], across, None) + dot(high[here], low[on], across, None)
        for b in range(a, blocks):
            out_ref[at : at + LANES, :] = strip[:, (b - a) * LANES : (b - a + 1) * LANES]
            at += LANES
    rounded = block_ref[...].astype(BF16)
    proj = dot(rounded, high, across, None) + dot(rounded, low, across, None)
    factors = proj.shape[0]
    for b in range(blocks):
        out_ref[at : at + factors, :] = proj[:, b * LANES : (b + 1) * LANES]
        at += factors
    if at < out_ref.shape[0]:
        out_ref[at:, :] = jnp.zeros((out_ref.shape[0] - at, LANES), F32)


def inverse_lower(gram):
    k = gram.shape[0]
    size = 8
    row = lax.broadcasted_iota(jnp.int32, (k, LANES), 0)
    lane = lax.broadcasted_iota(jnp.int32, (k, LANES), 1)
    both = jnp.concatenate([gram, jnp.zeros((k, LANES - k), F32)], axis=1)
    both = jnp.where(lane == row + k, 1.0, both)
    for i in range(0, k, size):
        columns = [jnp.broadcast_to(both[:, i + q : i + q + 1], (k, LANES)) for q in range(size)]
        lines = [both[i + q : i + q + 1, :] for q in range(size)]
        inner = {(q, p): columns[q][i + p : i + p + 1, :] for q in range(size) for p in range(q, size)}
        update = jnp.zeros((k, LANES), F32)
        for q in range(size):
            inverse = 1.0 / inner[q, q]
            later = range(q + 1, size)
            ratio = {p: inner[q, p] * inverse for p in later}
            for p in later:
                for r in range(p, size):
                    inner[p, r] -= ratio[p] * inner[q, r]
            for p in later:
                lines[p] -= ratio[p] * lines[q]
                columns[p] -= columns[q] * ratio[p]
            update += jnp.where(row > i + q, columns[q] * inverse, 0.0) * lines[q]
        both -= update
    pivots = jnp.sum(jnp.where(lane == row, both, 0.0), axis=1, keepdims=True)
    return (both * lax.rsqrt(pivots))[:, k : 2 * k]


def iterate_kernel(assets, got_ref, scaled_ref, out_ref, high_ref, low_ref):
    total = scaled_ref.shape[0]
    factors = out_ref.shape[1]
    blocks = total // LANES
    at = 0
    for a, b in tiles_of(total):
        rows, columns = slice(a * LANES, (a + 1) * LANES), slice(b * LANES, (b + 1) * LANES)
        tile = got_ref[at : at + LANES, :]
        high_ref[rows, columns], low_ref[rows, columns] = split(tile)
        if a != b:
            high_ref[columns, rows], low_ref[columns, rows] = split(tile.T)
        at += LANES
    proj = jnp.concatenate([got_ref[at + b * factors : at + (b + 1) * factors, :] for b in range(blocks)], axis=1)
    inward = ((1,), (0,))
    for step in range(ITERS):
        high, low = split(proj)
        stacked = dot(jnp.concatenate([high, low], axis=0), high_ref[...], inward, None)
        moved = stacked[:factors] + (stacked[factors:] + dot(high, low_ref[...], inward, None))
        gram = dot(moved, proj, ((1,), (1,))) * (1.0 / assets)
        proj = dot(inverse_lower(gram), moved if step < ITERS - 1 else proj, inward)
    loadings = dot3(proj, scaled_ref[...], inward).astype(BF16)
    out_ref[...] = jnp.broadcast_to(loadings[None], out_ref.shape)


def unpack_kernel(got_ref, out_ref):
    windows, _, width = out_ref.shape
    parts = width // LANES
    for w in range(windows):
        for j in range(parts):
            out_ref[w, :, j * LANES : (j + 1) * LANES] = got_ref[w * parts + j].astype(F32)


def on_device(returns, starts, start_block):
    windows, days, width = returns.shape
    factors = start_block.shape[1]
    parts = width // LANES
    rows = windows * parts
    sides = lax.axis_size(("cols", "sub"))
    total = days * rows
    assets = width * sides
    w, j = lax.axis_index("window"), lax.axis_index("part")
    row = w * parts + j

    packed = pl.pallas_call(
        pack_kernel,
        out_shape=jax.ShapeDtypeStruct((rows, days + EXTRA, LANES), BF16),
        in_specs=[SMEM, VMEM, VMEM],
        out_specs=VMEM,
        compiler_params=PARAMS,
        name="pack",
    )(row[None], returns, starts)
    got = lax.all_to_all(packed, ("window", "part"), 0, 0, tiled=True)

    filled = len(tiles_of(total)) * LANES + factors * total // LANES
    unit = 8 * sides * parts
    height = (filled + unit - 1) // unit * unit
    scaled, partial = pl.pallas_call(
        gram_kernel,
        out_shape=(
            jax.ShapeDtypeStruct((total, LANES), F32),
            jax.ShapeDtypeStruct((height, LANES), F32),
        ),
        in_specs=[VMEM] * 3,
        out_specs=(VMEM, VMEM),
        compiler_params=PARAMS,
        name="gram",
    )(
        got,
        lax.dynamic_slice(starts, (w, j * LANES), (1, LANES)),
        lax.dynamic_slice(start_block, (w, 0, j * LANES), (1, factors, LANES))[0],
    )

    own = lax.all_to_all(partial.reshape(sides, height // sides, LANES), ("cols", "sub"), 0, 0, tiled=True)
    own = own.sum(axis=0).reshape(parts, height // sides // parts, LANES)
    own = lax.all_to_all(own, "part", 0, 0, tiled=True).sum(axis=0)
    own = lax.all_to_all(jnp.broadcast_to(own[None], (parts, *own.shape)), "part", 0, 0, tiled=True)
    whole = lax.all_gather(own.reshape(height // sides, LANES), ("cols", "sub"), tiled=True)

    sent = pl.pallas_call(
        functools.partial(iterate_kernel, assets),
        out_shape=jax.ShapeDtypeStruct((rows, factors, LANES), BF16),
        in_specs=[VMEM, VMEM],
        out_specs=VMEM,
        scratch_shapes=[pltpu.VMEM((total, total), BF16)] * 2,
        compiler_params=PARAMS,
        name="iterate",
    )(whole, scaled)
    got = lax.all_to_all(sent, ("window", "part"), 0, 0, tiled=True)
    return pl.pallas_call(
        unpack_kernel,
        out_shape=jax.ShapeDtypeStruct((windows, factors, width), F32),
        in_specs=[VMEM],
        out_specs=VMEM,
        compiler_params=PARAMS,
        name="unpack",
    )(got)


def solution(mesh):
    groups, rows, cols, sub = (mesh.shape[name] for name in ("groups", "rows", "cols", "sub"))

    def whole(returns, starts, start_block):
        windows = returns.shape[0] // groups
        split = Mesh(
            mesh.devices.reshape(groups, windows, rows // windows, cols, sub),
            ("groups", "window", "part", "cols", "sub"),
        )
        placed = (
            P("groups", ("window", "part"), ("cols", "sub")),
            P("groups", ("cols", "sub")),
            P("groups", None, ("cols", "sub")),
        )
        return jax.shard_map(
            on_device,
            mesh=split,
            in_specs=placed,
            out_specs=P("groups", None, ("cols", "sub")),
            check_vma=False,
        )(returns, starts, start_block)

    return whole
```

```python
import functools

import jax
import jax.numpy as jnp
from jax import lax
from jax.experimental import pallas as pl
from jax.experimental.pallas import tpu as pltpu
from jax.sharding import Mesh
from jax.sharding import PartitionSpec as P

ITERS = 3
LANES = 128
HALF = LANES // 2
NEAR = 4
EXTRA = 8
F32 = jnp.float32
BF16 = jnp.bfloat16
HIGHEST = lax.Precision.HIGHEST
VMEM = pl.BlockSpec(memory_space=pltpu.VMEM)
SMEM = pl.BlockSpec(memory_space=pltpu.SMEM)
PARAMS = pltpu.CompilerParams(vmem_limit_bytes=16 << 20)


def dot(a, b, dims, precision=HIGHEST):
    return lax.dot_general(a, b, (dims, ((), ())), precision=precision, preferred_element_type=F32)


def split(a):
    high = a.astype(BF16)
    return high, (a - high.astype(F32)).astype(BF16)


def dot3(a, b, dims):
    (ah, al), (bh, bl) = split(a), split(b)
    return dot(ah, bh, dims, None) + (dot(al, bh, dims, None) + dot(ah, bl, dims, None))


def pack_kernel(where_ref, returns_ref, starts_ref, out_ref):
    windows, days, width = returns_ref.shape
    parts = width // LANES
    day = lax.broadcasted_iota(jnp.int32, (days, width), 0) + where_ref[0] * days
    row = lax.broadcasted_iota(jnp.int32, (EXTRA, width), 0)
    for w in range(windows):
        live = day >= starts_ref[w : w + 1, :]
        kept = jnp.where(live, returns_ref[w], 0.0)
        number = jnp.sum(live.astype(F32), axis=0, keepdims=True)
        shift = jnp.sum(kept, axis=0, keepdims=True) / jnp.maximum(number, 1.0)
        high = shift.astype(BF16).astype(F32)
        middle = (shift - high).astype(BF16).astype(F32)
        low = (shift - high - middle).astype(BF16).astype(F32)
        shift = high + middle + low
        rest = jnp.where(live, kept - shift, 0.0).astype(BF16)
        carried = jnp.where(row == 0, high, jnp.where(row == 1, middle, jnp.where(row == 2, low, 0.0))).astype(BF16)
        for j in range(parts):
            at = slice(j * LANES, (j + 1) * LANES)
            out_ref[w * parts + j, 0:days, :] = rest[:, at]
            out_ref[w * parts + j, days : days + EXTRA, :] = carried[:, at]


def gram_kernel(got_ref, starts_ref, block_ref, scaled_ref, out_ref):
    sources, rows, _ = got_ref.shape
    days = rows - EXTRA
    total = sources * days
    starts = starts_ref[...]
    got = got_ref[...].astype(F32)
    shift = jnp.sum(got[:, days:, :], axis=1, keepdims=True)
    values = (got[:, :days, :] + shift).reshape(total, LANES)
    live = lax.broadcasted_iota(jnp.int32, (total, LANES), 0) >= starts
    counts = (total - starts).astype(F32)
    mean = jnp.sum(jnp.where(live, values, 0.0), axis=0, keepdims=True) / counts
    centered = jnp.where(live, values - mean, 0.0)
    squares = jnp.sum(centered * centered, axis=0, keepdims=True)
    scaled = centered * lax.rsqrt(squares + 1.0)
    scaled_ref[...] = scaled
    high, low = split(scaled)
    blocks = total // LANES
    across = ((1,), (1,))
    rounded = block_ref[...].astype(BF16)
    proj = dot(rounded, high, across, None) + dot(rounded, low, across, None)
    rest = []
    at = 0

    def put(tile):
        nonlocal at
        out_ref[at : at + tile.shape[0], :] = tile
        at += tile.shape[0]

    for a in range(blocks):
        here, on = slice(a * LANES, (a + 1) * LANES), slice(a * LANES, total)
        strip = dot(high[here], high[on], across, None)
        strip += dot(low[here], high[on], across, None) + dot(high[here], low[on], across, None)
        put(strip[:HALF, :LANES])
        rest.append(strip[HALF:, :LANES])
        for b in range(1, blocks - a):
            put(strip[:, b * LANES : (b + 1) * LANES])
    left = lax.broadcasted_iota(jnp.int32, (HALF, LANES), 1) < HALF
    for a in range(0, blocks, 2):
        put(jnp.where(left, pltpu.roll(rest[a], HALF, 1), rest[a + 1]))
    for b in range(blocks):
        put(proj[:, b * LANES : (b + 1) * LANES])
    if at < out_ref.shape[0]:
        out_ref[at:, :] = jnp.zeros((out_ref.shape[0] - at, LANES), F32)


def inverse_lower(gram):
    k = gram.shape[0]
    size = 8
    row = lax.broadcasted_iota(jnp.int32, (k, LANES), 0)
    lane = lax.broadcasted_iota(jnp.int32, (k, LANES), 1)
    both = jnp.concatenate([gram, jnp.zeros((k, LANES - k), F32)], axis=1)
    both = jnp.where(lane == row + k, 1.0, both)
    for i in range(0, k, size):
        columns = [jnp.broadcast_to(both[:, i + q : i + q + 1], (k, LANES)) for q in range(size)]
        lines = [both[i + q : i + q + 1, :] for q in range(size)]
        inner = {(q, p): columns[q][i + p : i + p + 1, :] for q in range(size) for p in range(q, size)}
        update = jnp.zeros((k, LANES), F32)
        for q in range(size):
            inverse = 1.0 / inner[q, q]
            later = range(q + 1, size)
            ratio = {p: inner[q, p] * inverse for p in later}
            for p in later:
                for r in range(p, size):
                    inner[p, r] -= ratio[p] * inner[q, r]
            for p in later:
                lines[p] -= ratio[p] * lines[q]
                columns[p] -= columns[q] * ratio[p]
            update += jnp.where(row > i + q, columns[q] * inverse, 0.0) * lines[q]
        both -= update
    pivots = jnp.sum(jnp.where(lane == row, both, 0.0), axis=1, keepdims=True)
    return (both * lax.rsqrt(pivots))[:, k : 2 * k]


def iterate_kernel(assets, got_ref, scaled_ref, out_ref, high_ref, low_ref):
    total = scaled_ref.shape[0]
    factors = out_ref.shape[1]
    blocks = total // LANES
    row = lax.broadcasted_iota(jnp.int32, (LANES, LANES), 0)
    lane = lax.broadcasted_iota(jnp.int32, (LANES, LANES), 1)
    at = 0

    def take(rows):
        nonlocal at
        at += rows
        return got_ref[at - rows : at, :]

    tops = []
    for a in range(blocks):
        here = slice(a * LANES, (a + 1) * LANES)
        tops.append(take(HALF))
        for b in range(a + 1, blocks):
            there = slice(b * LANES, (b + 1) * LANES)
            tile = take(LANES)
            high_ref[here, there], low_ref[here, there] = split(tile)
            high_ref[there, here], low_ref[there, here] = split(tile.T)
    for a in range(0, blocks, 2):
        pair = take(HALF)
        for c, rest in ((a, pltpu.roll(pair, HALF, 1)), (a + 1, pair)):
            here = slice(c * LANES, (c + 1) * LANES)
            tile = jnp.concatenate([tops[c], rest], axis=0)
            tile = jnp.where((row >= HALF) & (lane < HALF), tile.T, tile)
            high_ref[here, here], low_ref[here, here] = split(tile)
    proj = jnp.concatenate([take(factors) for b in range(blocks)], axis=1)
    inward = ((1,), (0,))
    for step in range(ITERS):
        high, low = split(proj)
        stacked = dot(jnp.concatenate([high, low], axis=0), high_ref[...], inward, None)
        moved = stacked[:factors] + (stacked[factors:] + dot(high, low_ref[...], inward, None))
        gram = dot(moved, proj, ((1,), (1,))) * (1.0 / assets)
        proj = dot(inverse_lower(gram), moved if step < ITERS - 1 else proj, inward)
    loadings = dot3(proj, scaled_ref[...], inward).astype(BF16)
    out_ref[...] = jnp.broadcast_to(loadings[None], out_ref.shape)


def unpack_kernel(got_ref, out_ref):
    windows, _, width = out_ref.shape
    near, blocks = got_ref.shape[:2]
    for w in range(windows):
        for j in range(width // LANES):
            block = w * (blocks // windows) + j // near
            out_ref[w, :, j * LANES : (j + 1) * LANES] = got_ref[j % near, block].astype(F32)


def on_device(returns, starts, start_block):
    windows, days, width = returns.shape
    factors = start_block.shape[1]
    parts = width // LANES
    rows = windows * parts
    cols, sub = lax.axis_size("cols"), lax.axis_size("sub")
    sides = cols * sub
    total = days * rows
    assets = width * sides
    part = ("far", "near")
    w, j = lax.axis_index("window"), lax.axis_index(part)
    row = w * parts + j

    packed = pl.pallas_call(
        pack_kernel,
        out_shape=jax.ShapeDtypeStruct((rows, days + EXTRA, LANES), BF16),
        in_specs=[SMEM, VMEM, VMEM],
        out_specs=VMEM,
        name="pack",
    )(row[None], returns, starts)
    got = lax.all_to_all(packed, ("window", *part), 0, 0, tiled=True)

    blocks = total // LANES
    filled = blocks * (blocks - 1) // 2 * LANES + blocks // 2 * 3 * HALF + factors * blocks
    height = (filled + 8 * sides - 1) // (8 * sides) * (8 * sides)
    scaled, partial = pl.pallas_call(
        gram_kernel,
        out_shape=(
            jax.ShapeDtypeStruct((total, LANES), F32),
            jax.ShapeDtypeStruct((height, LANES), F32),
        ),
        in_specs=[VMEM] * 3,
        out_specs=(VMEM, VMEM),
        compiler_params=PARAMS,
        name="gram",
    )(
        got,
        lax.dynamic_slice(starts, (w, j * LANES), (1, LANES)),
        lax.dynamic_slice(start_block, (w, 0, j * LANES), (1, factors, LANES))[0],
    )

    share = height // sides
    padded = (share + 8 * parts - 1) // (8 * parts) * (8 * parts)
    own = lax.all_to_all(partial.reshape(sides, share, LANES), ("sub", "cols"), 0, 0, tiled=True).sum(axis=0)
    own = jnp.pad(own, ((0, padded - share), (0, 0))).reshape(parts, padded // parts, LANES)
    own = lax.all_to_all(own, part, 0, 0, tiled=True).sum(axis=0)
    own = lax.all_to_all(jnp.broadcast_to(own[None], (parts, *own.shape)), part, 0, 0, tiled=True)
    own = own.reshape(padded, LANES)[:share]
    own = lax.all_to_all(jnp.broadcast_to(own[None], (cols, share, LANES)), "cols", 0, 0, tiled=True)
    whole = lax.all_gather(own.reshape(cols * share, LANES), "sub", tiled=True)

    far = windows * parts // NEAR
    sent = pl.pallas_call(
        functools.partial(iterate_kernel, assets),
        out_shape=jax.ShapeDtypeStruct((far, factors, LANES), BF16),
        in_specs=[VMEM, VMEM],
        out_specs=VMEM,
        scratch_shapes=[pltpu.VMEM((total, total), BF16)] * 2,
        compiler_params=PARAMS,
        name="iterate",
    )(whole, scaled)
    got = lax.all_to_all(sent, ("window", "far"), 0, 0, tiled=True)
    got = lax.all_to_all(jnp.broadcast_to(got[None], (NEAR, *got.shape)), "near", 0, 0, tiled=True)
    return pl.pallas_call(
        unpack_kernel,
        out_shape=jax.ShapeDtypeStruct((windows, factors, width), F32),
        in_specs=[VMEM],
        out_specs=VMEM,
        compiler_params=PARAMS,
        name="unpack",
    )(got)


def solution(mesh):
    groups, rows, cols, sub = (mesh.shape[name] for name in ("groups", "rows", "cols", "sub"))

    def whole(returns, starts, start_block):
        windows = returns.shape[0] // groups
        split = Mesh(
            mesh.devices.reshape(groups, windows, rows // windows // NEAR, NEAR, cols, sub),
            ("groups", "window", "far", "near", "cols", "sub"),
        )
        placed = (
            P("groups", ("window", "far", "near"), ("cols", "sub")),
            P("groups", ("cols", "sub")),
            P("groups", None, ("cols", "sub")),
        )
        return jax.shard_map(
            on_device,
            mesh=split,
            in_specs=placed,
            out_specs=P("groups", None, ("cols", "sub")),
            check_vma=False,
        )(returns, starts, start_block)

    return whole
```

```python
import functools

import jax
import jax.numpy as jnp
from jax import lax
from jax.experimental import pallas as pl
from jax.experimental.pallas import tpu as pltpu
from jax.sharding import Mesh
from jax.sharding import PartitionSpec as P

ITERS = 3
LANES = 128
HALF = LANES // 2
NEAR = 4
EIGHT = 8
QUAD = 4
F32 = jnp.float32
BF16 = jnp.bfloat16
HIGHEST = lax.Precision.HIGHEST
VMEM = pl.BlockSpec(memory_space=pltpu.VMEM)
SMEM = pl.BlockSpec(memory_space=pltpu.SMEM)
PARAMS = pltpu.CompilerParams(vmem_limit_bytes=16 << 20)


def dot(a, b, dims, precision=HIGHEST):
    return lax.dot_general(a, b, (dims, ((), ())), precision=precision, preferred_element_type=F32)


def split(a):
    high = a.astype(BF16)
    return high, (a - high.astype(F32)).astype(BF16)


def dot3(a, b, dims):
    (ah, al), (bh, bl) = split(a), split(b)
    return dot(ah, bh, dims, None) + (dot(al, bh, dims, None) + dot(ah, bl, dims, None))


def pack_kernel(where_ref, returns_ref, starts_ref, out_ref):
    windows, days, width = returns_ref.shape
    parts = width // LANES
    day = lax.broadcasted_iota(jnp.int32, (days, width), 0) + where_ref[0] * days
    row = lax.broadcasted_iota(jnp.int32, (QUAD, width), 0)
    for w in range(windows):
        live = day >= starts_ref[w : w + 1, :]
        kept = jnp.where(live, returns_ref[w], 0.0)
        number = jnp.sum(live.astype(F32), axis=0, keepdims=True)
        shift = jnp.sum(kept, axis=0, keepdims=True) / jnp.maximum(number, 1.0)
        high = shift.astype(BF16).astype(F32)
        middle = (shift - high).astype(BF16).astype(F32)
        low = (shift - high - middle).astype(BF16).astype(F32)
        shift = high + middle + low
        rest = jnp.where(live, kept - shift, 0.0)
        carried = jnp.where(row == 0, high, jnp.where(row == 1, middle, jnp.where(row == 2, low, 0.0)))
        blocks = [rest[i : i + QUAD] for i in range(0, days, QUAD)] + [carried]
        for i, block in enumerate(blocks):
            block = block.astype(BF16)
            for j in range(parts):
                out_ref[w * parts + j, :, i * LANES : (i + 1) * LANES] = block[:, j * LANES : (j + 1) * LANES]


def gram_kernel(where_ref, got_ref, starts_ref, block_ref, scaled_ref, out_ref):
    sources = got_ref.shape[0]
    days = (got_ref.shape[2] // LANES - 1) * QUAD
    total = sources * days
    parts = sources // starts_ref.shape[0]
    w = where_ref[0] // parts
    own = pl.ds(pl.multiple_of(where_ref[0] % parts * LANES, LANES), LANES)
    starts = starts_ref[:, own]
    starts = jnp.sum(jnp.where(lax.broadcasted_iota(jnp.int32, starts.shape, 0) == w, starts, 0), axis=0, keepdims=True)
    got = got_ref[...].astype(F32)
    lanes = [got[:, :, at : at + LANES] for at in range(0, got.shape[2], LANES)]
    shift = jnp.sum(lanes[-1], axis=1, keepdims=True)
    eights = [jnp.concatenate(lanes[i : i + 2], axis=1) + shift for i in range(0, len(lanes) - 1, 2)]
    values = jnp.concatenate([eight.reshape(sources * EIGHT, LANES) for eight in eights], axis=0)
    row = lax.broadcasted_iota(jnp.int32, (total, LANES), 0)
    eight, source = row // (sources * EIGHT), row % (sources * EIGHT) // EIGHT
    live = source * days + eight * EIGHT + row % EIGHT >= starts
    counts = (total - starts).astype(F32)
    mean = jnp.sum(jnp.where(live, values, 0.0), axis=0, keepdims=True) / counts
    centered = jnp.where(live, values - mean, 0.0)
    squares = jnp.sum(centered * centered, axis=0, keepdims=True)
    scaled = centered * lax.rsqrt(squares + 1.0)
    scaled_ref[...] = scaled
    high, low = split(scaled)
    blocks = total // LANES
    across = ((1,), (1,))
    rounded = block_ref[w, :, own].astype(BF16)
    proj = dot(rounded, high, across, None) + dot(rounded, low, across, None)
    rest = []
    at = 0

    def put(tile):
        nonlocal at
        out_ref[at : at + tile.shape[0], :] = tile
        at += tile.shape[0]

    for a in range(blocks):
        here, on = slice(a * LANES, (a + 1) * LANES), slice(a * LANES, total)
        strip = dot(high[here], high[on], across, None)
        strip += dot(low[here], high[on], across, None) + dot(high[here], low[on], across, None)
        put(strip[:HALF, :LANES])
        rest.append(strip[HALF:, :LANES])
        for b in range(1, blocks - a):
            put(strip[:, b * LANES : (b + 1) * LANES])
    left = lax.broadcasted_iota(jnp.int32, (HALF, LANES), 1) < HALF
    for a in range(0, blocks, 2):
        put(jnp.where(left, pltpu.roll(rest[a], HALF, 1), rest[a + 1]))
    for b in range(blocks):
        put(proj[:, b * LANES : (b + 1) * LANES])
    if at < out_ref.shape[0]:
        out_ref[at:, :] = jnp.zeros((out_ref.shape[0] - at, LANES), F32)


def inverse_lower(gram):
    k = gram.shape[0]
    size = 8
    row = lax.broadcasted_iota(jnp.int32, (k, LANES), 0)
    lane = lax.broadcasted_iota(jnp.int32, (k, LANES), 1)
    both = jnp.concatenate([gram, jnp.zeros((k, LANES - k), F32)], axis=1)
    both = jnp.where(lane == row + k, 1.0, both)
    for i in range(0, k, size):
        columns = [jnp.broadcast_to(both[:, i + q : i + q + 1], (k, LANES)) for q in range(size)]
        lines = [both[i + q : i + q + 1, :] for q in range(size)]
        inner = {(q, p): columns[q][i + p : i + p + 1, :] for q in range(size) for p in range(q, size)}
        update = jnp.zeros((k, LANES), F32)
        for q in range(size):
            inverse = 1.0 / inner[q, q]
            later = range(q + 1, size)
            ratio = {p: inner[q, p] * inverse for p in later}
            for p in later:
                for r in range(p, size):
                    inner[p, r] -= ratio[p] * inner[q, r]
            for p in later:
                lines[p] -= ratio[p] * lines[q]
                columns[p] -= columns[q] * ratio[p]
            update += jnp.where(row > i + q, columns[q] * inverse, 0.0) * lines[q]
        both -= update
    pivots = jnp.sum(jnp.where(lane == row, both, 0.0), axis=1, keepdims=True)
    return (both * lax.rsqrt(pivots))[:, k : 2 * k]


def iterate_kernel(assets, got_ref, scaled_ref, out_ref, high_ref, low_ref):
    total = scaled_ref.shape[0]
    factors = out_ref.shape[1]
    blocks = total // LANES
    row = lax.broadcasted_iota(jnp.int32, (LANES, LANES), 0)
    lane = lax.broadcasted_iota(jnp.int32, (LANES, LANES), 1)
    at = 0

    def take(rows):
        nonlocal at
        at += rows
        return got_ref[at - rows : at, :]

    tops = []
    for a in range(blocks):
        here = slice(a * LANES, (a + 1) * LANES)
        tops.append(take(HALF))
        for b in range(a + 1, blocks):
            there = slice(b * LANES, (b + 1) * LANES)
            tile = take(LANES)
            high_ref[here, there], low_ref[here, there] = split(tile)
            high_ref[there, here], low_ref[there, here] = split(tile.T)
    for a in range(0, blocks, 2):
        pair = take(HALF)
        for c, rest in ((a, pltpu.roll(pair, HALF, 1)), (a + 1, pair)):
            here = slice(c * LANES, (c + 1) * LANES)
            tile = jnp.concatenate([tops[c], rest], axis=0)
            tile = jnp.where((row >= HALF) & (lane < HALF), tile.T, tile)
            high_ref[here, here], low_ref[here, here] = split(tile)
    proj = jnp.concatenate([take(factors) for b in range(blocks)], axis=1)
    inward = ((1,), (0,))
    for step in range(ITERS):
        high, low = split(proj)
        stacked = dot(jnp.concatenate([high, low], axis=0), high_ref[...], inward, None)
        moved = stacked[:factors] + (stacked[factors:] + dot(high, low_ref[...], inward, None))
        gram = dot(moved, proj, ((1,), (1,))) * (1.0 / assets)
        proj = dot(inverse_lower(gram), moved if step < ITERS - 1 else proj, inward)
    loadings = dot3(proj, scaled_ref[...], inward).astype(BF16)
    out_ref[...] = jnp.broadcast_to(loadings[None], out_ref.shape)


def unpack_kernel(got_ref, out_ref):
    windows, _, width = out_ref.shape
    near, blocks = got_ref.shape[:2]
    for w in range(windows):
        for j in range(width // LANES):
            block = w * (blocks // windows) + j // near
            out_ref[w, :, j * LANES : (j + 1) * LANES] = got_ref[j % near, block].astype(F32)


def on_device(returns, starts, start_block):
    windows, days, width = returns.shape
    factors = start_block.shape[1]
    parts = width // LANES
    rows = windows * parts
    cols, sub = lax.axis_size("cols"), lax.axis_size("sub")
    sides = cols * sub
    total = days * rows
    assets = width * sides
    part = ("far", "near")
    row = lax.axis_index("window") * parts + lax.axis_index(part)

    packed = pl.pallas_call(
        pack_kernel,
        out_shape=jax.ShapeDtypeStruct((rows, QUAD, (days // QUAD + 1) * LANES), BF16),
        in_specs=[SMEM, VMEM, VMEM],
        out_specs=VMEM,
        name="pack",
    )(row[None], returns, starts)
    got = lax.all_to_all(packed, ("window", *part), 0, 0, tiled=True)

    blocks = total // LANES
    filled = blocks * (blocks - 1) // 2 * LANES + blocks // 2 * 3 * HALF + factors * blocks
    height = (filled + 8 * sides - 1) // (8 * sides) * (8 * sides)
    scaled, partial = pl.pallas_call(
        gram_kernel,
        out_shape=(
            jax.ShapeDtypeStruct((total, LANES), F32),
            jax.ShapeDtypeStruct((height, LANES), F32),
        ),
        in_specs=[SMEM, VMEM, VMEM, VMEM],
        out_specs=(VMEM, VMEM),
        compiler_params=PARAMS,
        name="gram",
    )(row[None], got, starts, start_block)

    share = height // sides
    padded = (share + 8 * parts - 1) // (8 * parts) * (8 * parts)
    own = lax.all_to_all(partial.reshape(sides, share, LANES), ("sub", "cols"), 0, 0, tiled=True).sum(axis=0)
    own = jnp.pad(own, ((0, padded - share), (0, 0))).reshape(parts, padded // parts, LANES)
    own = lax.all_to_all(own, part, 0, 0, tiled=True).sum(axis=0)
    own = lax.all_to_all(jnp.broadcast_to(own[None], (parts, *own.shape)), part, 0, 0, tiled=True)
    own = own.reshape(padded, LANES)[:share]
    own = lax.all_to_all(jnp.broadcast_to(own[None], (cols, share, LANES)), "cols", 0, 0, tiled=True)
    whole = lax.all_gather(own.reshape(cols * share, LANES), "sub", tiled=True)

    far = windows * parts // NEAR
    sent = pl.pallas_call(
        functools.partial(iterate_kernel, assets),
        out_shape=jax.ShapeDtypeStruct((far, factors, LANES), BF16),
        in_specs=[VMEM, VMEM],
        out_specs=VMEM,
        scratch_shapes=[pltpu.VMEM((total, total), BF16)] * 2,
        compiler_params=PARAMS,
        name="iterate",
    )(whole, scaled)
    got = lax.all_to_all(sent, ("window", "far"), 0, 0, tiled=True)
    got = lax.all_to_all(jnp.broadcast_to(got[None], (NEAR, *got.shape)), "near", 0, 0, tiled=True)
    return pl.pallas_call(
        unpack_kernel,
        out_shape=jax.ShapeDtypeStruct((windows, factors, width), F32),
        in_specs=[VMEM],
        out_specs=VMEM,
        compiler_params=PARAMS,
        name="unpack",
    )(got)


def solution(mesh):
    groups, rows, cols, sub = (mesh.shape[name] for name in ("groups", "rows", "cols", "sub"))

    def whole(returns, starts, start_block):
        windows = returns.shape[0] // groups
        split = Mesh(
            mesh.devices.reshape(groups, windows, rows // windows // NEAR, NEAR, cols, sub),
            ("groups", "window", "far", "near", "cols", "sub"),
        )
        placed = (
            P("groups", ("window", "far", "near"), ("cols", "sub")),
            P("groups", ("cols", "sub")),
            P("groups", None, ("cols", "sub")),
        )
        return jax.shard_map(
            on_device,
            mesh=split,
            in_specs=placed,
            out_specs=P("groups", None, ("cols", "sub")),
            check_vma=False,
        )(returns, starts, start_block)

    return whole
```

```python
import functools

import jax
import jax.numpy as jnp
from jax import lax
from jax.experimental import pallas as pl
from jax.experimental.pallas import tpu as pltpu
from jax.sharding import Mesh
from jax.sharding import PartitionSpec as P

ITERS = 3
LANES = 128
HALF = LANES // 2
NEAR = 4
EIGHT = 8
QUAD = 4
F32 = jnp.float32
BF16 = jnp.bfloat16
HIGHEST = lax.Precision.HIGHEST
VMEM = pl.BlockSpec(memory_space=pltpu.VMEM)
SMEM = pl.BlockSpec(memory_space=pltpu.SMEM)
PARAMS = pltpu.CompilerParams(vmem_limit_bytes=16 << 20)


def dot(a, b, dims, precision=HIGHEST):
    return lax.dot_general(a, b, (dims, ((), ())), precision=precision, preferred_element_type=F32)


def split(a):
    high = a.astype(BF16)
    return high, (a - high.astype(F32)).astype(BF16)


def dot3(a, b, dims):
    (ah, al), (bh, bl) = split(a), split(b)
    return dot(ah, bh, dims, None) + (dot(al, bh, dims, None) + dot(ah, bl, dims, None))


def pack_kernel(where_ref, returns_ref, starts_ref, out_ref):
    windows, days, width = returns_ref.shape
    parts = width // LANES
    day = lax.broadcasted_iota(jnp.int32, (days, width), 0) + where_ref[0] * days
    row = lax.broadcasted_iota(jnp.int32, (QUAD, width), 0)
    for w in range(windows):
        live = day >= starts_ref[w : w + 1, :]
        kept = jnp.where(live, returns_ref[w], 0.0)
        number = jnp.sum(live.astype(F32), axis=0, keepdims=True)
        shift = jnp.sum(kept, axis=0, keepdims=True) / jnp.maximum(number, 1.0)
        high = shift.astype(BF16).astype(F32)
        middle = (shift - high).astype(BF16).astype(F32)
        low = (shift - high - middle).astype(BF16).astype(F32)
        shift = high + middle + low
        rest = jnp.where(live, kept - shift, 0.0)
        carried = jnp.where(row == 0, high, jnp.where(row == 1, middle, jnp.where(row == 2, low, 0.0)))
        blocks = [rest[i : i + QUAD] for i in range(0, days, QUAD)] + [carried]
        for i, block in enumerate(blocks):
            block = block.astype(BF16)
            for j in range(parts):
                out_ref[w * parts + j, :, i * LANES : (i + 1) * LANES] = block[:, j * LANES : (j + 1) * LANES]


def scale_kernel(where_ref, got_ref, starts_ref, block_ref, out_ref):
    sources = got_ref.shape[0]
    days = (got_ref.shape[2] // LANES - 1) * QUAD
    total = sources * days
    parts = sources // starts_ref.shape[0]
    w = where_ref[0] // parts
    own = pl.ds(pl.multiple_of(where_ref[0] % parts * LANES, LANES), LANES)
    starts = starts_ref[:, own]
    starts = jnp.sum(jnp.where(lax.broadcasted_iota(jnp.int32, starts.shape, 0) == w, starts, 0), axis=0, keepdims=True)
    got = got_ref[...].astype(F32)
    lanes = [got[:, :, at : at + LANES] for at in range(0, got.shape[2], LANES)]
    shift = jnp.sum(lanes[-1], axis=1, keepdims=True)
    eights = [jnp.concatenate(lanes[i : i + 2], axis=1) + shift for i in range(0, len(lanes) - 1, 2)]
    values = jnp.concatenate([eight.reshape(sources * EIGHT, LANES) for eight in eights], axis=0)
    row = lax.broadcasted_iota(jnp.int32, (total, LANES), 0)
    eight, source = row // (sources * EIGHT), row % (sources * EIGHT) // EIGHT
    live = source * days + eight * EIGHT + row % EIGHT >= starts
    counts = (total - starts).astype(F32)
    mean = jnp.sum(jnp.where(live, values, 0.0), axis=0, keepdims=True) / counts
    centered = jnp.where(live, values - mean, 0.0)
    squares = jnp.sum(centered * centered, axis=0, keepdims=True)
    scaled = centered * lax.rsqrt(squares + 1.0)
    out_ref[0:total, :] = scaled
    out_ref[total:, :] = block_ref[w, :, own].astype(BF16).astype(F32)


def gram_kernel(where_ref, both_ref, out_ref, all_ref):
    cores, rows, _ = both_ref.shape
    total = rows // LANES * LANES
    both = jnp.concatenate([both_ref[c] for c in range(cores)], axis=1)
    high, low = split(both[:total])
    rounded = both[total:].astype(BF16)
    blocks = total // LANES
    across = ((1,), (1,))
    proj = dot(rounded, high, across, None) + dot(rounded, low, across, None)
    rest = []
    at = 0

    def put(tile):
        nonlocal at
        all_ref[at : at + tile.shape[0], :] = tile
        at += tile.shape[0]

    for a in range(blocks):
        here, on = slice(a * LANES, (a + 1) * LANES), slice(a * LANES, total)
        strip = dot(high[here], high[on], across, None)
        strip += dot(low[here], high[on], across, None) + dot(high[here], low[on], across, None)
        put(strip[:HALF, :LANES])
        rest.append(strip[HALF:, :LANES])
        for b in range(1, blocks - a):
            put(strip[:, b * LANES : (b + 1) * LANES])
    left = lax.broadcasted_iota(jnp.int32, (HALF, LANES), 1) < HALF
    for a in range(0, blocks, 2):
        put(jnp.where(left, pltpu.roll(rest[a], HALF, 1), rest[a + 1]))
    for b in range(blocks):
        put(proj[:, b * LANES : (b + 1) * LANES])
    if at < all_ref.shape[0]:
        all_ref[at:, :] = jnp.zeros((all_ref.shape[0] - at, LANES), F32)
    share = out_ref.shape[0]
    out_ref[...] = all_ref[pl.ds(pl.multiple_of(where_ref[0] * share, EIGHT), share), :]


def inverse_lower(gram):
    k = gram.shape[0]
    size = 8
    row = lax.broadcasted_iota(jnp.int32, (k, LANES), 0)
    lane = lax.broadcasted_iota(jnp.int32, (k, LANES), 1)
    both = jnp.concatenate([gram, jnp.zeros((k, LANES - k), F32)], axis=1)
    both = jnp.where(lane == row + k, 1.0, both)
    for i in range(0, k, size):
        columns = [jnp.broadcast_to(both[:, i + q : i + q + 1], (k, LANES)) for q in range(size)]
        lines = [both[i + q : i + q + 1, :] for q in range(size)]
        inner = {(q, p): columns[q][i + p : i + p + 1, :] for q in range(size) for p in range(q, size)}
        update = jnp.zeros((k, LANES), F32)
        for q in range(size):
            inverse = 1.0 / inner[q, q]
            later = range(q + 1, size)
            ratio = {p: inner[q, p] * inverse for p in later}
            for p in later:
                for r in range(p, size):
                    inner[p, r] -= ratio[p] * inner[q, r]
            for p in later:
                lines[p] -= ratio[p] * lines[q]
                columns[p] -= columns[q] * ratio[p]
            update += jnp.where(row > i + q, columns[q] * inverse, 0.0) * lines[q]
        both -= update
    pivots = jnp.sum(jnp.where(lane == row, both, 0.0), axis=1, keepdims=True)
    return (both * lax.rsqrt(pivots))[:, k : 2 * k]


def iterate_kernel(assets, got_ref, scaled_ref, out_ref, high_ref, low_ref):
    factors = out_ref.shape[1]
    total = scaled_ref.shape[0] - factors
    blocks = total // LANES
    row = lax.broadcasted_iota(jnp.int32, (LANES, LANES), 0)
    lane = lax.broadcasted_iota(jnp.int32, (LANES, LANES), 1)
    at = 0

    def take(rows):
        nonlocal at
        at += rows
        return got_ref[at - rows : at, :]

    tops = []
    for a in range(blocks):
        here = slice(a * LANES, (a + 1) * LANES)
        tops.append(take(HALF))
        for b in range(a + 1, blocks):
            there = slice(b * LANES, (b + 1) * LANES)
            tile = take(LANES)
            high_ref[here, there], low_ref[here, there] = split(tile)
            high_ref[there, here], low_ref[there, here] = split(tile.T)
    for a in range(0, blocks, 2):
        pair = take(HALF)
        for c, rest in ((a, pltpu.roll(pair, HALF, 1)), (a + 1, pair)):
            here = slice(c * LANES, (c + 1) * LANES)
            tile = jnp.concatenate([tops[c], rest], axis=0)
            tile = jnp.where((row >= HALF) & (lane < HALF), tile.T, tile)
            high_ref[here, here], low_ref[here, here] = split(tile)
    proj = jnp.concatenate([take(factors) for b in range(blocks)], axis=1)
    inward = ((1,), (0,))
    for step in range(ITERS):
        high, low = split(proj)
        stacked = dot(jnp.concatenate([high, low], axis=0), high_ref[...], inward, None)
        moved = stacked[:factors] + (stacked[factors:] + dot(high, low_ref[...], inward, None))
        gram = dot(moved, proj, ((1,), (1,))) * (1.0 / assets)
        proj = dot(inverse_lower(gram), moved if step < ITERS - 1 else proj, inward)
    loadings = dot3(proj, scaled_ref[0:total, :], inward).astype(BF16)
    out_ref[...] = jnp.broadcast_to(loadings[None], out_ref.shape)


def unpack_kernel(got_ref, out_ref):
    windows, _, width = out_ref.shape
    near, blocks = got_ref.shape[:2]
    for w in range(windows):
        for j in range(width // LANES):
            block = w * (blocks // windows) + j // near
            out_ref[w, :, j * LANES : (j + 1) * LANES] = got_ref[j % near, block].astype(F32)


def on_device(returns, starts, start_block):
    windows, days, width = returns.shape
    factors = start_block.shape[1]
    parts = width // LANES
    rows = windows * parts
    cols, sub = lax.axis_size("cols"), lax.axis_size("sub")
    sides = cols * sub
    total = days * rows
    assets = width * sides
    part = ("far", "near")
    row = lax.axis_index("window") * parts + lax.axis_index(part)

    packed = pl.pallas_call(
        pack_kernel,
        out_shape=jax.ShapeDtypeStruct((rows, QUAD, (days // QUAD + 1) * LANES), BF16),
        in_specs=[SMEM, VMEM, VMEM],
        out_specs=VMEM,
        name="pack",
    )(row[None], returns, starts)
    got = lax.all_to_all(packed, ("window", *part), 0, 0, tiled=True)

    blocks = total // LANES
    filled = blocks * (blocks - 1) // 2 * LANES + blocks // 2 * 3 * HALF + factors * blocks
    height = (filled + 8 * sides - 1) // (8 * sides) * (8 * sides)
    scaled = pl.pallas_call(
        scale_kernel,
        out_shape=jax.ShapeDtypeStruct((total + factors, LANES), F32),
        in_specs=[SMEM, VMEM, VMEM, VMEM],
        out_specs=VMEM,
        compiler_params=PARAMS,
        name="scale",
    )(row[None], got, starts, start_block)
    both = lax.all_gather(scaled, "sub")
    partial = pl.pallas_call(
        gram_kernel,
        out_shape=jax.ShapeDtypeStruct((height // sub, LANES), F32),
        in_specs=[SMEM, VMEM],
        out_specs=VMEM,
        scratch_shapes=[pltpu.VMEM((height, LANES), F32)],
        compiler_params=PARAMS,
        name="gram",
    )(lax.axis_index("sub")[None], both)

    share = height // sides
    own = lax.all_to_all(partial.reshape(cols, share, LANES), "cols", 0, 0, tiled=True).sum(axis=0)
    own = lax.all_to_all(jnp.broadcast_to(own[None], (NEAR, share, LANES)), "near", 0, 0, tiled=True).sum(axis=0)
    own = lax.all_gather(own, "far").sum(axis=0)
    own = lax.all_to_all(jnp.broadcast_to(own[None], (cols, share, LANES)), "cols", 0, 0, tiled=True)
    whole = lax.all_gather(own.reshape(cols * share, LANES), "sub", tiled=True)

    far = windows * parts // NEAR
    sent = pl.pallas_call(
        functools.partial(iterate_kernel, assets),
        out_shape=jax.ShapeDtypeStruct((far, factors, LANES), BF16),
        in_specs=[VMEM, VMEM],
        out_specs=VMEM,
        scratch_shapes=[pltpu.VMEM((total, total), BF16)] * 2,
        compiler_params=PARAMS,
        name="iterate",
    )(whole, scaled)
    got = lax.all_to_all(sent, ("window", "far"), 0, 0, tiled=True)
    got = lax.all_to_all(jnp.broadcast_to(got[None], (NEAR, *got.shape)), "near", 0, 0, tiled=True)
    return pl.pallas_call(
        unpack_kernel,
        out_shape=jax.ShapeDtypeStruct((windows, factors, width), F32),
        in_specs=[VMEM],
        out_specs=VMEM,
        compiler_params=PARAMS,
        name="unpack",
    )(got)


def solution(mesh):
    groups, rows, cols, sub = (mesh.shape[name] for name in ("groups", "rows", "cols", "sub"))

    def whole(returns, starts, start_block):
        windows = returns.shape[0] // groups
        split = Mesh(
            mesh.devices.reshape(groups, windows, rows // windows // NEAR, NEAR, cols, sub),
            ("groups", "window", "far", "near", "cols", "sub"),
        )
        placed = (
            P("groups", ("window", "far", "near"), ("cols", "sub")),
            P("groups", ("cols", "sub")),
            P("groups", None, ("cols", "sub")),
        )
        return jax.shard_map(
            on_device,
            mesh=split,
            in_specs=placed,
            out_specs=P("groups", None, ("cols", "sub")),
            check_vma=False,
        )(returns, starts, start_block)

    return whole
```

```python
import functools

import jax
import jax.numpy as jnp
from jax import lax
from jax.experimental import pallas as pl
from jax.experimental.pallas import tpu as pltpu
from jax.sharding import Mesh
from jax.sharding import PartitionSpec as P

ITERS = 3
LANES = 128
HALF = LANES // 2
NEAR = 4
EIGHT = 8
QUAD = 4
F32 = jnp.float32
BF16 = jnp.bfloat16
HIGHEST = lax.Precision.HIGHEST
VMEM = pl.BlockSpec(memory_space=pltpu.VMEM)
SMEM = pl.BlockSpec(memory_space=pltpu.SMEM)
PARAMS = pltpu.CompilerParams(vmem_limit_bytes=16 << 20)


def dot(a, b, dims, precision=HIGHEST):
    return lax.dot_general(a, b, (dims, ((), ())), precision=precision, preferred_element_type=F32)


def split(a):
    high = a.astype(BF16)
    return high, (a - high.astype(F32)).astype(BF16)


def dot3(a, b, dims):
    (ah, al), (bh, bl) = split(a), split(b)
    return dot(ah, bh, dims, None) + (dot(al, bh, dims, None) + dot(ah, bl, dims, None))


def pack_kernel(where_ref, returns_ref, starts_ref, out_ref):
    windows, days, width = returns_ref.shape
    parts = width // LANES
    day = lax.broadcasted_iota(jnp.int32, (days, width), 0) + where_ref[0] * days
    row = lax.broadcasted_iota(jnp.int32, (QUAD, width), 0)
    for w in range(windows):
        live = day >= starts_ref[w : w + 1, :]
        kept = jnp.where(live, returns_ref[w], 0.0)
        number = jnp.sum(live.astype(F32), axis=0, keepdims=True)
        shift = jnp.sum(kept, axis=0, keepdims=True) / jnp.maximum(number, 1.0)
        high = shift.astype(BF16).astype(F32)
        middle = (shift - high).astype(BF16).astype(F32)
        low = (shift - high - middle).astype(BF16).astype(F32)
        shift = high + middle + low
        rest = jnp.where(live, kept - shift, 0.0)
        carried = jnp.where(row == 0, high, jnp.where(row == 1, middle, jnp.where(row == 2, low, 0.0)))
        blocks = [rest[i : i + QUAD] for i in range(0, days, QUAD)] + [carried]
        for i, block in enumerate(blocks):
            block = block.astype(BF16)
            for j in range(parts):
                out_ref[w * parts + j, :, i * LANES : (i + 1) * LANES] = block[:, j * LANES : (j + 1) * LANES]


def scale_kernel(where_ref, got_ref, starts_ref, block_ref, out_ref):
    sources = got_ref.shape[0]
    days = (got_ref.shape[2] // LANES - 1) * QUAD
    total = sources * days
    parts = sources // starts_ref.shape[0]
    w = where_ref[0] // parts
    own = pl.ds(pl.multiple_of(where_ref[0] % parts * LANES, LANES), LANES)
    starts = starts_ref[:, own]
    starts = jnp.sum(jnp.where(lax.broadcasted_iota(jnp.int32, starts.shape, 0) == w, starts, 0), axis=0, keepdims=True)
    got = got_ref[...].astype(F32)
    lanes = [got[:, :, at : at + LANES] for at in range(0, got.shape[2], LANES)]
    shift = jnp.sum(lanes[-1], axis=1, keepdims=True)
    eights = [jnp.concatenate(lanes[i : i + 2], axis=1) + shift for i in range(0, len(lanes) - 1, 2)]
    values = jnp.concatenate([eight.reshape(sources * EIGHT, LANES) for eight in eights], axis=0)
    row = lax.broadcasted_iota(jnp.int32, (total, LANES), 0)
    eight, source = row // (sources * EIGHT), row % (sources * EIGHT) // EIGHT
    live = source * days + eight * EIGHT + row % EIGHT >= starts
    counts = (total - starts).astype(F32)
    mean = jnp.sum(jnp.where(live, values, 0.0), axis=0, keepdims=True) / counts
    centered = jnp.where(live, values - mean, 0.0)
    squares = jnp.sum(centered * centered, axis=0, keepdims=True)
    scaled = centered * lax.rsqrt(squares + 1.0)
    out_ref[0:total, :] = scaled
    out_ref[total:, :] = block_ref[w, :, own].astype(BF16).astype(F32)


def gram_kernel(where_ref, both_ref, out_ref, all_ref):
    cores, rows, _ = both_ref.shape
    total = rows // LANES * LANES
    both = jnp.concatenate([both_ref[c] for c in range(cores)], axis=1)
    high, low = split(both[:total])
    rounded = both[total:].astype(BF16)
    blocks = total // LANES
    across = ((1,), (1,))
    proj = dot(rounded, high, across, None) + dot(rounded, low, across, None)
    rest = []
    at = 0

    def put(tile):
        nonlocal at
        all_ref[at : at + tile.shape[0], :] = tile
        at += tile.shape[0]

    for a in range(blocks):
        here, on = slice(a * LANES, (a + 1) * LANES), slice(a * LANES, total)
        strip = dot(high[here], high[on], across, None)
        strip += dot(low[here], high[on], across, None) + dot(high[here], low[on], across, None)
        put(strip[:HALF, :LANES])
        rest.append(strip[HALF:, :LANES])
        for b in range(1, blocks - a):
            put(strip[:, b * LANES : (b + 1) * LANES])
    left = lax.broadcasted_iota(jnp.int32, (HALF, LANES), 1) < HALF
    for a in range(0, blocks, 2):
        put(jnp.where(left, pltpu.roll(rest[a], HALF, 1), rest[a + 1]))
    for b in range(blocks):
        put(proj[:, b * LANES : (b + 1) * LANES])
    if at < all_ref.shape[0]:
        all_ref[at:, :] = jnp.zeros((all_ref.shape[0] - at, LANES), F32)
    share = out_ref.shape[0]
    out_ref[...] = all_ref[pl.ds(pl.multiple_of(where_ref[0] * share, EIGHT), share), :]


def inverse_lower(gram):
    k = gram.shape[0]
    size = 8
    row = lax.broadcasted_iota(jnp.int32, (k, LANES), 0)
    lane = lax.broadcasted_iota(jnp.int32, (k, LANES), 1)
    both = jnp.concatenate([gram, jnp.zeros((k, LANES - k), F32)], axis=1)
    both = jnp.where(lane == row + k, 1.0, both)
    for i in range(0, k, size):
        columns = [jnp.broadcast_to(both[:, i + q : i + q + 1], (k, LANES)) for q in range(size)]
        lines = [both[i + q : i + q + 1, :] for q in range(size)]
        inner = {(q, p): columns[q][i + p : i + p + 1, :] for q in range(size) for p in range(q, size)}
        update = jnp.zeros((k, LANES), F32)
        for q in range(size):
            inverse = 1.0 / inner[q, q]
            later = range(q + 1, size)
            ratio = {p: inner[q, p] * inverse for p in later}
            for p in later:
                for r in range(p, size):
                    inner[p, r] -= ratio[p] * inner[q, r]
            for p in later:
                lines[p] -= ratio[p] * lines[q]
                columns[p] -= columns[q] * ratio[p]
            update += jnp.where(row > i + q, columns[q] * inverse, 0.0) * lines[q]
        both -= update
    pivots = jnp.sum(jnp.where(lane == row, both, 0.0), axis=1, keepdims=True)
    return (both * lax.rsqrt(pivots))[:, k : 2 * k]


def iterate_kernel(assets, got_ref, scaled_ref, out_ref, high_ref, low_ref):
    factors = out_ref.shape[1]
    total = scaled_ref.shape[0] - factors
    blocks = total // LANES
    row = lax.broadcasted_iota(jnp.int32, (LANES, LANES), 0)
    lane = lax.broadcasted_iota(jnp.int32, (LANES, LANES), 1)
    at = 0

    def take(rows):
        nonlocal at
        at += rows
        return got_ref[at - rows : at, :]

    tops = []
    for a in range(blocks):
        here = slice(a * LANES, (a + 1) * LANES)
        tops.append(take(HALF))
        for b in range(a + 1, blocks):
            there = slice(b * LANES, (b + 1) * LANES)
            tile = take(LANES)
            high_ref[here, there], low_ref[here, there] = split(tile)
            high_ref[there, here], low_ref[there, here] = split(tile.T)
    for a in range(0, blocks, 2):
        pair = take(HALF)
        for c, rest in ((a, pltpu.roll(pair, HALF, 1)), (a + 1, pair)):
            here = slice(c * LANES, (c + 1) * LANES)
            tile = jnp.concatenate([tops[c], rest], axis=0)
            tile = jnp.where((row >= HALF) & (lane < HALF), tile.T, tile)
            high_ref[here, here], low_ref[here, here] = split(tile)
    proj = jnp.concatenate([take(factors) for b in range(blocks)], axis=1)
    inward = ((1,), (0,))
    for step in range(ITERS):
        high, low = split(proj)
        stacked = dot(jnp.concatenate([high, low], axis=0), high_ref[...], inward, None)
        moved = stacked[:factors] + (stacked[factors:] + dot(high, low_ref[...], inward, None))
        gram = dot(moved, proj, ((1,), (1,))) * (1.0 / assets)
        proj = dot(inverse_lower(gram), moved if step < ITERS - 1 else proj, inward)
    loadings = dot3(proj, scaled_ref[0:total, :], inward).astype(BF16)
    out_ref[...] = jnp.broadcast_to(loadings[None], out_ref.shape)


def unpack_kernel(got_ref, out_ref):
    windows, _, width = out_ref.shape
    near, blocks = got_ref.shape[:2]
    for w in range(windows):
        for j in range(width // LANES):
            block = w * (blocks // windows) + j // near
            out_ref[w, :, j * LANES : (j + 1) * LANES] = got_ref[j % near, block].astype(F32)


def on_device(returns, starts, start_block):
    windows, days, width = returns.shape
    factors = start_block.shape[1]
    parts = width // LANES
    rows = windows * parts
    cols, sub = lax.axis_size("cols"), lax.axis_size("sub")
    sides = cols * sub
    total = days * rows
    assets = width * sides
    part, quad, block = ("far", "mid", "near"), ("mid", "near"), ("near", "cols")
    row = lax.axis_index("window") * parts + lax.axis_index(part)

    packed = pl.pallas_call(
        pack_kernel,
        out_shape=jax.ShapeDtypeStruct((rows, QUAD, (days // QUAD + 1) * LANES), BF16),
        in_specs=[SMEM, VMEM, VMEM],
        out_specs=VMEM,
        name="pack",
    )(row[None], returns, starts)
    got = lax.all_to_all(packed, ("window", *part), 0, 0, tiled=True)

    blocks = total // LANES
    filled = blocks * (blocks - 1) // 2 * LANES + blocks // 2 * 3 * HALF + factors * blocks
    unit = EIGHT * sub * lax.axis_size(block)
    height = (filled + unit - 1) // unit * unit
    scaled = pl.pallas_call(
        scale_kernel,
        out_shape=jax.ShapeDtypeStruct((total + factors, LANES), F32),
        in_specs=[SMEM, VMEM, VMEM, VMEM],
        out_specs=VMEM,
        compiler_params=PARAMS,
        name="scale",
    )(row[None], got, starts, start_block)
    both = lax.all_gather(scaled, "sub")
    partial = pl.pallas_call(
        gram_kernel,
        out_shape=jax.ShapeDtypeStruct((height // sub, LANES), F32),
        in_specs=[SMEM, VMEM],
        out_specs=VMEM,
        scratch_shapes=[pltpu.VMEM((height, LANES), F32)],
        compiler_params=PARAMS,
        name="gram",
    )(lax.axis_index("sub")[None], both)

    pieces = lax.axis_size(block)
    share = height // sub // pieces
    own = lax.all_to_all(partial.reshape(pieces, share, LANES), block, 0, 0, tiled=True).sum(axis=0)
    own = lax.all_gather(own, "mid").sum(axis=0)
    own = lax.all_gather(own, "far").sum(axis=0)
    own = lax.all_to_all(jnp.broadcast_to(own[None], (pieces, share, LANES)), block, 0, 0, tiled=True)
    whole = lax.all_gather(own.reshape(height // sub, LANES), "sub", tiled=True)

    far = windows * parts // NEAR
    sent = pl.pallas_call(
        functools.partial(iterate_kernel, assets),
        out_shape=jax.ShapeDtypeStruct((far, factors, LANES), BF16),
        in_specs=[VMEM, VMEM],
        out_specs=VMEM,
        scratch_shapes=[pltpu.VMEM((total, total), BF16)] * 2,
        compiler_params=PARAMS,
        name="iterate",
    )(whole, scaled)
    got = lax.all_to_all(sent, ("window", "far"), 0, 0, tiled=True)
    got = lax.all_to_all(jnp.broadcast_to(got[None], (NEAR, *got.shape)), quad, 0, 0, tiled=True)
    return pl.pallas_call(
        unpack_kernel,
        out_shape=jax.ShapeDtypeStruct((windows, factors, width), F32),
        in_specs=[VMEM],
        out_specs=VMEM,
        compiler_params=PARAMS,
        name="unpack",
    )(got)


def solution(mesh):
    groups, rows, cols, sub = (mesh.shape[name] for name in ("groups", "rows", "cols", "sub"))

    def whole(returns, starts, start_block):
        windows = returns.shape[0] // groups
        split = Mesh(
            mesh.devices.reshape(groups, windows, rows // windows // NEAR, NEAR // 2, 2, cols, sub),
            ("groups", "window", "far", "mid", "near", "cols", "sub"),
        )
        placed = (
            P("groups", ("window", "far", "mid", "near"), ("cols", "sub")),
            P("groups", ("cols", "sub")),
            P("groups", None, ("cols", "sub")),
        )
        return jax.shard_map(
            on_device,
            mesh=split,
            in_specs=placed,
            out_specs=P("groups", None, ("cols", "sub")),
            check_vma=False,
        )(returns, starts, start_block)

    return whole
```

```python
import functools

import jax
import jax.numpy as jnp
from jax import lax
from jax.experimental import pallas as pl
from jax.experimental.pallas import tpu as pltpu
from jax.sharding import Mesh
from jax.sharding import PartitionSpec as P

ITERS = 3
LANES = 128
HALF = LANES // 2
NEAR = 4
EIGHT = 8
QUAD = 4
F32 = jnp.float32
BF16 = jnp.bfloat16
HIGHEST = lax.Precision.HIGHEST
VMEM = pl.BlockSpec(memory_space=pltpu.VMEM)
HBM = pl.BlockSpec(memory_space=pltpu.HBM)
SMEM = pl.BlockSpec(memory_space=pltpu.SMEM)
PARAMS = pltpu.CompilerParams(vmem_limit_bytes=16 << 20)


def dot(a, b, dims, precision=HIGHEST):
    return lax.dot_general(a, b, (dims, ((), ())), precision=precision, preferred_element_type=F32)


def split(a):
    high = a.astype(BF16)
    return high, (a - high.astype(F32)).astype(BF16)


def dot3(a, b, dims):
    (ah, al), (bh, bl) = split(a), split(b)
    return dot(ah, bh, dims, None) + (dot(al, bh, dims, None) + dot(ah, bl, dims, None))


def pack_kernel(where_ref, returns_hbm, starts_hbm, out_ref, returns_ref, starts_ref, arrived):
    windows, days, width = returns_ref.shape
    parts = width // LANES
    copies = [pltpu.make_async_copy(starts_hbm, starts_ref, arrived.at[windows])]
    copies += [pltpu.make_async_copy(returns_hbm.at[w], returns_ref.at[w], arrived.at[w]) for w in range(windows)]
    for copy in copies:
        copy.start()
    day = lax.broadcasted_iota(jnp.int32, (days, width), 0) + where_ref[0] * days
    row = lax.broadcasted_iota(jnp.int32, (QUAD, width), 0)
    copies[0].wait()
    for w in range(windows):
        copies[w + 1].wait()
        live = day >= starts_ref[w : w + 1, :]
        kept = jnp.where(live, returns_ref[w], 0.0)
        number = jnp.sum(live.astype(F32), axis=0, keepdims=True)
        shift = jnp.sum(kept, axis=0, keepdims=True) / jnp.maximum(number, 1.0)
        high = shift.astype(BF16).astype(F32)
        middle = (shift - high).astype(BF16).astype(F32)
        low = (shift - high - middle).astype(BF16).astype(F32)
        shift = high + middle + low
        rest = jnp.where(live, kept - shift, 0.0)
        carried = jnp.where(row == 0, high, jnp.where(row == 1, middle, jnp.where(row == 2, low, 0.0)))
        blocks = [rest[i : i + QUAD] for i in range(0, days, QUAD)] + [carried]
        for i, block in enumerate(blocks):
            block = block.astype(BF16)
            for j in range(parts):
                out_ref[w * parts + j, :, i * LANES : (i + 1) * LANES] = block[:, j * LANES : (j + 1) * LANES]


def scale_kernel(where_ref, got_ref, starts_ref, block_ref, out_ref):
    sources = got_ref.shape[0]
    days = (got_ref.shape[2] // LANES - 1) * QUAD
    total = sources * days
    parts = sources // starts_ref.shape[0]
    w = where_ref[0] // parts
    own = pl.ds(pl.multiple_of(where_ref[0] % parts * LANES, LANES), LANES)
    starts = starts_ref[:, own]
    starts = jnp.sum(jnp.where(lax.broadcasted_iota(jnp.int32, starts.shape, 0) == w, starts, 0), axis=0, keepdims=True)
    got = got_ref[...].astype(F32)
    lanes = [got[:, :, at : at + LANES] for at in range(0, got.shape[2], LANES)]
    shift = jnp.sum(lanes[-1], axis=1, keepdims=True)
    eights = [jnp.concatenate(lanes[i : i + 2], axis=1) + shift for i in range(0, len(lanes) - 1, 2)]
    values = jnp.concatenate([eight.reshape(sources * EIGHT, LANES) for eight in eights], axis=0)
    row = lax.broadcasted_iota(jnp.int32, (total, LANES), 0)
    eight, source = row // (sources * EIGHT), row % (sources * EIGHT) // EIGHT
    live = source * days + eight * EIGHT + row % EIGHT >= starts
    counts = (total - starts).astype(F32)
    mean = jnp.sum(jnp.where(live, values, 0.0), axis=0, keepdims=True) / counts
    centered = jnp.where(live, values - mean, 0.0)
    squares = jnp.sum(centered * centered, axis=0, keepdims=True)
    scaled = centered * lax.rsqrt(squares + 1.0)
    out_ref[0:total, :] = scaled
    out_ref[total:, :] = block_ref[w, :, own].astype(BF16).astype(F32)


def gram_kernel(where_ref, both_ref, out_ref, all_ref):
    cores, rows, _ = both_ref.shape
    total = rows // LANES * LANES
    both = jnp.concatenate([both_ref[c] for c in range(cores)], axis=1)
    high, low = split(both[:total])
    rounded = both[total:].astype(BF16)
    blocks = total // LANES
    across = ((1,), (1,))
    proj = dot(rounded, high, across, None) + dot(rounded, low, across, None)
    rest = []
    at = 0

    def put(tile):
        nonlocal at
        all_ref[at : at + tile.shape[0], :] = tile
        at += tile.shape[0]

    for a in range(blocks):
        here, on = slice(a * LANES, (a + 1) * LANES), slice(a * LANES, total)
        strip = dot(high[here], high[on], across, None)
        strip += dot(low[here], high[on], across, None) + dot(high[here], low[on], across, None)
        put(strip[:HALF, :LANES])
        rest.append(strip[HALF:, :LANES])
        for b in range(1, blocks - a):
            put(strip[:, b * LANES : (b + 1) * LANES])
    left = lax.broadcasted_iota(jnp.int32, (HALF, LANES), 1) < HALF
    for a in range(0, blocks, 2):
        put(jnp.where(left, pltpu.roll(rest[a], HALF, 1), rest[a + 1]))
    for b in range(blocks):
        put(proj[:, b * LANES : (b + 1) * LANES])
    if at < all_ref.shape[0]:
        all_ref[at:, :] = jnp.zeros((all_ref.shape[0] - at, LANES), F32)
    share = out_ref.shape[0]
    out_ref[...] = all_ref[pl.ds(pl.multiple_of(where_ref[0] * share, EIGHT), share), :]


def inverse_lower(gram):
    k = gram.shape[0]
    size = 8
    row = lax.broadcasted_iota(jnp.int32, (k, LANES), 0)
    lane = lax.broadcasted_iota(jnp.int32, (k, LANES), 1)
    both = jnp.concatenate([gram, jnp.zeros((k, LANES - k), F32)], axis=1)
    both = jnp.where(lane == row + k, 1.0, both)
    for i in range(0, k, size):
        columns = [jnp.broadcast_to(both[:, i + q : i + q + 1], (k, LANES)) for q in range(size)]
        lines = [both[i + q : i + q + 1, :] for q in range(size)]
        inner = {(q, p): columns[q][i + p : i + p + 1, :] for q in range(size) for p in range(q, size)}
        update = jnp.zeros((k, LANES), F32)
        for q in range(size):
            inverse = 1.0 / inner[q, q]
            later = range(q + 1, size)
            ratio = {p: inner[q, p] * inverse for p in later}
            for p in later:
                for r in range(p, size):
                    inner[p, r] -= ratio[p] * inner[q, r]
            for p in later:
                lines[p] -= ratio[p] * lines[q]
                columns[p] -= columns[q] * ratio[p]
            update += jnp.where(row > i + q, columns[q] * inverse, 0.0) * lines[q]
        both -= update
    pivots = jnp.sum(jnp.where(lane == row, both, 0.0), axis=1, keepdims=True)
    return (both * lax.rsqrt(pivots))[:, k : 2 * k]


def iterate_kernel(assets, got_ref, scaled_ref, out_ref, high_ref, low_ref):
    factors = out_ref.shape[1]
    total = scaled_ref.shape[0] - factors
    blocks = total // LANES
    row = lax.broadcasted_iota(jnp.int32, (LANES, LANES), 0)
    lane = lax.broadcasted_iota(jnp.int32, (LANES, LANES), 1)
    at = 0

    def take(rows):
        nonlocal at
        at += rows
        return got_ref[at - rows : at, :]

    tops = []
    for a in range(blocks):
        here = slice(a * LANES, (a + 1) * LANES)
        tops.append(take(HALF))
        for b in range(a + 1, blocks):
            there = slice(b * LANES, (b + 1) * LANES)
            tile = take(LANES)
            high_ref[here, there], low_ref[here, there] = split(tile)
            high_ref[there, here], low_ref[there, here] = split(tile.T)
    for a in range(0, blocks, 2):
        pair = take(HALF)
        for c, rest in ((a, pltpu.roll(pair, HALF, 1)), (a + 1, pair)):
            here = slice(c * LANES, (c + 1) * LANES)
            tile = jnp.concatenate([tops[c], rest], axis=0)
            tile = jnp.where((row >= HALF) & (lane < HALF), tile.T, tile)
            high_ref[here, here], low_ref[here, here] = split(tile)
    proj = jnp.concatenate([take(factors) for b in range(blocks)], axis=1)
    inward = ((1,), (0,))
    for step in range(ITERS):
        high, low = split(proj)
        stacked = dot(jnp.concatenate([high, low], axis=0), high_ref[...], inward, None)
        moved = stacked[:factors] + (stacked[factors:] + dot(high, low_ref[...], inward, None))
        gram = dot(moved, proj, ((1,), (1,))) * (1.0 / assets)
        proj = dot(inverse_lower(gram), moved if step < ITERS - 1 else proj, inward)
    loadings = dot3(proj, scaled_ref[0:total, :], inward).astype(BF16)
    out_ref[...] = jnp.broadcast_to(loadings[None], out_ref.shape)


def unpack_kernel(got_ref, out_ref):
    windows, _, width = out_ref.shape
    near, blocks = got_ref.shape[:2]
    for w in range(windows):
        for j in range(width // LANES):
            block = w * (blocks // windows) + j // near
            out_ref[w, :, j * LANES : (j + 1) * LANES] = got_ref[j % near, block].astype(F32)


def on_device(returns, starts, start_block):
    windows, days, width = returns.shape
    factors = start_block.shape[1]
    parts = width // LANES
    rows = windows * parts
    cols, sub = lax.axis_size("cols"), lax.axis_size("sub")
    sides = cols * sub
    total = days * rows
    assets = width * sides
    part, quad, block = ("far", "mid", "near"), ("mid", "near"), ("near", "cols")
    row = lax.axis_index("window") * parts + lax.axis_index(part)

    packed = pl.pallas_call(
        pack_kernel,
        out_shape=jax.ShapeDtypeStruct((rows, QUAD, (days // QUAD + 1) * LANES), BF16),
        in_specs=[SMEM, HBM, HBM],
        out_specs=VMEM,
        scratch_shapes=[
            pltpu.VMEM(returns.shape, F32),
            pltpu.VMEM(starts.shape, jnp.int32),
            pltpu.SemaphoreType.DMA((windows + 1,)),
        ],
        compiler_params=PARAMS,
        name="pack",
    )(row[None], returns, starts)
    got = lax.all_to_all(packed, ("window", *part), 0, 0, tiled=True)

    blocks = total // LANES
    filled = blocks * (blocks - 1) // 2 * LANES + blocks // 2 * 3 * HALF + factors * blocks
    unit = EIGHT * sub * lax.axis_size(block)
    height = (filled + unit - 1) // unit * unit
    scaled = pl.pallas_call(
        scale_kernel,
        out_shape=jax.ShapeDtypeStruct((total + factors, LANES), F32),
        in_specs=[SMEM, VMEM, VMEM, VMEM],
        out_specs=VMEM,
        compiler_params=PARAMS,
        name="scale",
    )(row[None], got, starts, start_block)
    both = lax.all_gather(scaled, "sub")
    partial = pl.pallas_call(
        gram_kernel,
        out_shape=jax.ShapeDtypeStruct((height // sub, LANES), F32),
        in_specs=[SMEM, VMEM],
        out_specs=VMEM,
        scratch_shapes=[pltpu.VMEM((height, LANES), F32)],
        compiler_params=PARAMS,
        name="gram",
    )(lax.axis_index("sub")[None], both)

    pieces = lax.axis_size(block)
    share = height // sub // pieces
    own = lax.all_to_all(partial.reshape(pieces, share, LANES), block, 0, 0, tiled=True).sum(axis=0)
    own = lax.all_gather(own, "mid").sum(axis=0)
    own = lax.all_gather(own, "far").sum(axis=0)
    own = lax.all_to_all(jnp.broadcast_to(own[None], (pieces, share, LANES)), block, 0, 0, tiled=True)
    whole = lax.all_gather(own.reshape(height // sub, LANES), "sub", tiled=True)

    far = windows * parts // NEAR
    sent = pl.pallas_call(
        functools.partial(iterate_kernel, assets),
        out_shape=jax.ShapeDtypeStruct((far, factors, LANES), BF16),
        in_specs=[VMEM, VMEM],
        out_specs=VMEM,
        scratch_shapes=[pltpu.VMEM((total, total), BF16)] * 2,
        compiler_params=PARAMS,
        name="iterate",
    )(whole, scaled)
    got = lax.all_to_all(sent, ("window", "far"), 0, 0, tiled=True)
    got = lax.all_to_all(jnp.broadcast_to(got[None], (NEAR, *got.shape)), quad, 0, 0, tiled=True)
    return pl.pallas_call(
        unpack_kernel,
        out_shape=jax.ShapeDtypeStruct((windows, factors, width), F32),
        in_specs=[VMEM],
        out_specs=VMEM,
        compiler_params=PARAMS,
        name="unpack",
    )(got)


def solution(mesh):
    groups, rows, cols, sub = (mesh.shape[name] for name in ("groups", "rows", "cols", "sub"))

    def whole(returns, starts, start_block):
        windows = returns.shape[0] // groups
        split = Mesh(
            mesh.devices.reshape(groups, windows, rows // windows // NEAR, NEAR // 2, 2, cols, sub),
            ("groups", "window", "far", "mid", "near", "cols", "sub"),
        )
        placed = (
            P("groups", ("window", "far", "mid", "near"), ("cols", "sub")),
            P("groups", ("cols", "sub")),
            P("groups", None, ("cols", "sub")),
        )
        return jax.shard_map(
            on_device,
            mesh=split,
            in_specs=placed,
            out_specs=P("groups", None, ("cols", "sub")),
            check_vma=False,
        )(returns, starts, start_block)

    return whole
```

```python
import functools

import jax
import jax.numpy as jnp
from jax import lax
from jax.experimental import pallas as pl
from jax.experimental.pallas import tpu as pltpu
from jax.sharding import Mesh
from jax.sharding import PartitionSpec as P

ITERS = 3
LANES = 128
HALF = LANES // 2
NEAR = 4
EIGHT = 8
QUAD = 4
F32 = jnp.float32
BF16 = jnp.bfloat16
HIGHEST = lax.Precision.HIGHEST
VMEM = pl.BlockSpec(memory_space=pltpu.VMEM)
HBM = pl.BlockSpec(memory_space=pltpu.HBM)
SMEM = pl.BlockSpec(memory_space=pltpu.SMEM)
PARAMS = pltpu.CompilerParams(vmem_limit_bytes=16 << 20)


def dot(a, b, dims, precision=HIGHEST):
    return lax.dot_general(a, b, (dims, ((), ())), precision=precision, preferred_element_type=F32)


def split(a):
    high = a.astype(BF16)
    return high, (a - high.astype(F32)).astype(BF16)


def dot3(a, b, dims):
    (ah, al), (bh, bl) = split(a), split(b)
    return dot(ah, bh, dims, None) + (dot(al, bh, dims, None) + dot(ah, bl, dims, None))


def pack_kernel(where_ref, returns_hbm, starts_hbm, out_ref, returns_ref, starts_ref, arrived):
    windows, days, width = returns_ref.shape
    parts = width // LANES
    copies = [pltpu.make_async_copy(starts_hbm, starts_ref, arrived.at[windows])]
    copies += [pltpu.make_async_copy(returns_hbm.at[w], returns_ref.at[w], arrived.at[w]) for w in range(windows)]
    for copy in copies:
        copy.start()
    day = lax.broadcasted_iota(jnp.int32, (days, width), 0) + where_ref[0] * days
    row = lax.broadcasted_iota(jnp.int32, (QUAD, width), 0)
    copies[0].wait()
    for w in range(windows):
        copies[w + 1].wait()
        live = day >= starts_ref[w : w + 1, :]
        kept = jnp.where(live, returns_ref[w], 0.0)
        number = jnp.sum(live.astype(F32), axis=0, keepdims=True)
        shift = jnp.sum(kept, axis=0, keepdims=True) / jnp.maximum(number, 1.0)
        high = shift.astype(BF16).astype(F32)
        middle = (shift - high).astype(BF16).astype(F32)
        low = (shift - high - middle).astype(BF16).astype(F32)
        shift = high + middle + low
        rest = jnp.where(live, kept - shift, 0.0)
        carried = jnp.where(row == 0, high, jnp.where(row == 1, middle, jnp.where(row == 2, low, 0.0)))
        blocks = [rest[i : i + QUAD] for i in range(0, days, QUAD)] + [carried]
        for i, block in enumerate(blocks):
            block = block.astype(BF16)
            for j in range(parts):
                out_ref[w * parts + j, :, i * LANES : (i + 1) * LANES] = block[:, j * LANES : (j + 1) * LANES]


def scale_kernel(where_ref, got_ref, starts_ref, block_ref, out_ref):
    sources = got_ref.shape[0]
    days = (got_ref.shape[2] // LANES - 1) * QUAD
    total = sources * days
    parts = sources // starts_ref.shape[0]
    w = where_ref[0] // parts
    own = pl.ds(pl.multiple_of(where_ref[0] % parts * LANES, LANES), LANES)
    starts = starts_ref[:, own]
    starts = jnp.sum(jnp.where(lax.broadcasted_iota(jnp.int32, starts.shape, 0) == w, starts, 0), axis=0, keepdims=True)
    got = got_ref[...].astype(F32)
    lanes = [got[:, :, at : at + LANES] for at in range(0, got.shape[2], LANES)]
    shift = jnp.sum(lanes[-1], axis=1, keepdims=True)
    eights = [jnp.concatenate(lanes[i : i + 2], axis=1) + shift for i in range(0, len(lanes) - 1, 2)]
    values = jnp.concatenate([eight.reshape(sources * EIGHT, LANES) for eight in eights], axis=0)
    row = lax.broadcasted_iota(jnp.int32, (total, LANES), 0)
    eight, source = row // (sources * EIGHT), row % (sources * EIGHT) // EIGHT
    live = source * days + eight * EIGHT + row % EIGHT >= starts
    counts = (total - starts).astype(F32)
    mean = jnp.sum(jnp.where(live, values, 0.0), axis=0, keepdims=True) / counts
    centered = jnp.where(live, values - mean, 0.0)
    squares = jnp.sum(centered * centered, axis=0, keepdims=True)
    scaled = centered * lax.rsqrt(squares + 1.0)
    out_ref[0:total, :] = scaled
    out_ref[total:, :] = block_ref[w, :, own].astype(BF16).astype(F32)


def gram_kernel(where_ref, both_ref, out_ref, all_ref):
    cores, rows, _ = both_ref.shape
    total = rows // LANES * LANES
    both = jnp.concatenate([both_ref[c] for c in range(cores)], axis=1)
    high, low = split(both[:total])
    rounded = both[total:].astype(BF16)
    blocks = total // LANES
    across = ((1,), (1,))
    proj = dot(rounded, high, across, None) + dot(rounded, low, across, None)
    rest = []
    at = 0

    def put(tile):
        nonlocal at
        all_ref[at : at + tile.shape[0], :] = tile
        at += tile.shape[0]

    for a in range(blocks):
        here, on = slice(a * LANES, (a + 1) * LANES), slice(a * LANES, total)
        strip = dot(high[here], high[on], across, None)
        strip += dot(low[here], high[on], across, None) + dot(high[here], low[on], across, None)
        put(strip[:HALF, :LANES])
        rest.append(strip[HALF:, :LANES])
        for b in range(1, blocks - a):
            put(strip[:, b * LANES : (b + 1) * LANES])
    left = lax.broadcasted_iota(jnp.int32, (HALF, LANES), 1) < HALF
    for a in range(0, blocks, 2):
        put(jnp.where(left, pltpu.roll(rest[a], HALF, 1), rest[a + 1]))
    for b in range(blocks):
        put(proj[:, b * LANES : (b + 1) * LANES])
    if at < all_ref.shape[0]:
        all_ref[at:, :] = jnp.zeros((all_ref.shape[0] - at, LANES), F32)
    share = out_ref.shape[0]
    out_ref[...] = all_ref[pl.ds(pl.multiple_of(where_ref[0] * share, EIGHT), share), :]


def inverse_lower(gram):
    k = gram.shape[0]
    size = 8
    row = lax.broadcasted_iota(jnp.int32, (k, LANES), 0)
    lane = lax.broadcasted_iota(jnp.int32, (k, LANES), 1)
    both = jnp.concatenate([gram, jnp.zeros((k, LANES - k), F32)], axis=1)
    both = jnp.where(lane == row + k, 1.0, both)
    for i in range(0, k, size):
        columns = [jnp.broadcast_to(both[:, i + q : i + q + 1], (k, LANES)) for q in range(size)]
        lines = [both[i + q : i + q + 1, :] for q in range(size)]
        inner = {(q, p): columns[q][i + p : i + p + 1, :] for q in range(size) for p in range(q, size)}
        update = jnp.zeros((k, LANES), F32)
        for q in range(size):
            inverse = 1.0 / inner[q, q]
            later = range(q + 1, size)
            ratio = {p: inner[q, p] * inverse for p in later}
            for p in later:
                for r in range(p, size):
                    inner[p, r] -= ratio[p] * inner[q, r]
            for p in later:
                lines[p] -= ratio[p] * lines[q]
                columns[p] -= columns[q] * ratio[p]
            update += jnp.where(row > i + q, columns[q] * inverse, 0.0) * lines[q]
        both -= update
    pivots = jnp.sum(jnp.where(lane == row, both, 0.0), axis=1, keepdims=True)
    return (both * lax.rsqrt(pivots))[:, k : 2 * k]


def iterate_kernel(assets, got_ref, scaled_ref, out_ref, high_ref, low_ref):
    factors = out_ref.shape[1]
    total = scaled_ref.shape[0] - factors
    blocks = total // LANES
    row = lax.broadcasted_iota(jnp.int32, (LANES, LANES), 0)
    lane = lax.broadcasted_iota(jnp.int32, (LANES, LANES), 1)
    at = 0

    def take(rows):
        nonlocal at
        at += rows
        return got_ref[at - rows : at, :]

    tops = []
    for a in range(blocks):
        here = slice(a * LANES, (a + 1) * LANES)
        tops.append(take(HALF))
        for b in range(a + 1, blocks):
            there = slice(b * LANES, (b + 1) * LANES)
            tile = take(LANES)
            high_ref[here, there], low_ref[here, there] = split(tile)
            high_ref[there, here], low_ref[there, here] = split(tile.T)
    for a in range(0, blocks, 2):
        pair = take(HALF)
        for c, rest in ((a, pltpu.roll(pair, HALF, 1)), (a + 1, pair)):
            here = slice(c * LANES, (c + 1) * LANES)
            tile = jnp.concatenate([tops[c], rest], axis=0)
            tile = jnp.where((row >= HALF) & (lane < HALF), tile.T, tile)
            high_ref[here, here], low_ref[here, here] = split(tile)
    proj = jnp.concatenate([take(factors) for b in range(blocks)], axis=1)
    inward = ((1,), (0,))
    for step in range(ITERS):
        high, low = split(proj)
        stacked = dot(jnp.concatenate([high, low], axis=0), high_ref[...], inward, None)
        moved = stacked[:factors] + (stacked[factors:] + dot(high, low_ref[...], inward, None))
        gram = dot(moved, proj, ((1,), (1,))) * (1.0 / assets)
        proj = dot(inverse_lower(gram), moved if step < ITERS - 1 else proj, inward)
    loadings = dot3(proj, scaled_ref[0:total, :], inward).astype(BF16)
    out_ref[...] = jnp.broadcast_to(loadings[None], out_ref.shape)


def unpack_kernel(got_ref, out_ref):
    windows, _, width = out_ref.shape
    near, mid, blocks = got_ref.shape[:3]
    for w in range(windows):
        for j in range(width // LANES):
            block = w * (blocks // windows) + j // (mid * near)
            out_ref[w, :, j * LANES : (j + 1) * LANES] = got_ref[j % near, j // near % mid, block].astype(F32)


def on_device(returns, starts, start_block):
    windows, days, width = returns.shape
    factors = start_block.shape[1]
    parts = width // LANES
    rows = windows * parts
    cols, sub = lax.axis_size("cols"), lax.axis_size("sub")
    sides = cols * sub
    total = days * rows
    assets = width * sides
    part, block = ("far", "mid", "near"), ("near", "cols")
    row = lax.axis_index("window") * parts + lax.axis_index(part)

    packed = pl.pallas_call(
        pack_kernel,
        out_shape=jax.ShapeDtypeStruct((rows, QUAD, (days // QUAD + 1) * LANES), BF16),
        in_specs=[SMEM, HBM, HBM],
        out_specs=VMEM,
        scratch_shapes=[
            pltpu.VMEM(returns.shape, F32),
            pltpu.VMEM(starts.shape, jnp.int32),
            pltpu.SemaphoreType.DMA((windows + 1,)),
        ],
        name="pack",
    )(row[None], returns, starts)
    got = lax.all_to_all(packed, ("window", *part), 0, 0, tiled=True)

    blocks = total // LANES
    filled = blocks * (blocks - 1) // 2 * LANES + blocks // 2 * 3 * HALF + factors * blocks
    unit = EIGHT * sub * lax.axis_size(block)
    height = (filled + unit - 1) // unit * unit
    scaled = pl.pallas_call(
        scale_kernel,
        out_shape=jax.ShapeDtypeStruct((total + factors, LANES), F32),
        in_specs=[SMEM, VMEM, VMEM, VMEM],
        out_specs=VMEM,
        compiler_params=PARAMS,
        name="scale",
    )(row[None], got, starts, start_block)
    both = lax.all_gather(scaled, "sub")
    partial = pl.pallas_call(
        gram_kernel,
        out_shape=jax.ShapeDtypeStruct((height // sub, LANES), F32),
        in_specs=[SMEM, VMEM],
        out_specs=VMEM,
        scratch_shapes=[pltpu.VMEM((height, LANES), F32)],
        compiler_params=PARAMS,
        name="gram",
    )(lax.axis_index("sub")[None], both)

    pieces = lax.axis_size(block)
    share = height // sub // pieces
    own = lax.all_to_all(partial.reshape(pieces, share, LANES), block, 0, 0, tiled=True).sum(axis=0)
    own = lax.all_gather(own, "mid").sum(axis=0)
    own = lax.all_gather(own, "far").sum(axis=0)
    own = lax.all_to_all(jnp.broadcast_to(own[None], (pieces, share, LANES)), block, 0, 0, tiled=True)
    whole = lax.all_gather(own.reshape(height // sub, LANES), "sub", tiled=True)

    far = windows * parts // NEAR
    sent = pl.pallas_call(
        functools.partial(iterate_kernel, assets),
        out_shape=jax.ShapeDtypeStruct((far, factors, LANES), BF16),
        in_specs=[VMEM, VMEM],
        out_specs=VMEM,
        scratch_shapes=[pltpu.VMEM((total, total), BF16)] * 2,
        compiler_params=PARAMS,
        name="iterate",
    )(whole, scaled)
    got = lax.all_to_all(sent, ("window", "far"), 0, 0, tiled=True)
    got = lax.all_gather(lax.all_gather(got, "mid"), "near")
    return pl.pallas_call(
        unpack_kernel,
        out_shape=jax.ShapeDtypeStruct((windows, factors, width), F32),
        in_specs=[VMEM],
        out_specs=VMEM,
        compiler_params=PARAMS,
        name="unpack",
    )(got)


def solution(mesh):
    groups, rows, cols, sub = (mesh.shape[name] for name in ("groups", "rows", "cols", "sub"))

    def whole(returns, starts, start_block):
        windows = returns.shape[0] // groups
        split = Mesh(
            mesh.devices.reshape(groups, windows, rows // windows // NEAR, NEAR // 2, 2, cols, sub),
            ("groups", "window", "far", "mid", "near", "cols", "sub"),
        )
        placed = (
            P("groups", ("window", "far", "mid", "near"), ("cols", "sub")),
            P("groups", ("cols", "sub")),
            P("groups", None, ("cols", "sub")),
        )
        return jax.shard_map(
            on_device,
            mesh=split,
            in_specs=placed,
            out_specs=P("groups", None, ("cols", "sub")),
            check_vma=False,
        )(returns, starts, start_block)

    return whole
```

```python
import functools

import jax
import jax.numpy as jnp
from jax import lax
from jax.experimental import pallas as pl
from jax.experimental.pallas import tpu as pltpu
from jax.sharding import Mesh
from jax.sharding import PartitionSpec as P

ITERS = 3
LANES = 128
ROWS = ("window", "far", "mid", "near")
HALF = LANES // 2
NEAR = 4
EIGHT = 8
QUAD = 4
F32 = jnp.float32
BF16 = jnp.bfloat16
HIGHEST = lax.Precision.HIGHEST
VMEM = pl.BlockSpec(memory_space=pltpu.VMEM)
PARAMS = pltpu.CompilerParams(vmem_limit_bytes=16 << 20)


def dot(a, b, dims, precision=HIGHEST):
    return lax.dot_general(a, b, (dims, ((), ())), precision=precision, preferred_element_type=F32)


def split(a):
    high = a.astype(BF16)
    return high, (a - high.astype(F32)).astype(BF16)


def dot3(a, b, dims):
    (ah, al), (bh, bl) = split(a), split(b)
    return dot(ah, bh, dims, None) + (dot(al, bh, dims, None) + dot(ah, bl, dims, None))


def pack_kernel(returns_ref, starts_ref, out_ref):
    windows, days, width = returns_ref.shape
    parts = width // LANES
    day = lax.broadcasted_iota(jnp.int32, (days, width), 0) + lax.axis_index(ROWS) * days
    row = lax.broadcasted_iota(jnp.int32, (QUAD, width), 0)
    for w in range(windows):
        live = day >= starts_ref[w : w + 1, :]
        kept = jnp.where(live, returns_ref[w], 0.0)
        number = jnp.sum(live.astype(F32), axis=0, keepdims=True)
        shift = jnp.sum(kept, axis=0, keepdims=True) / jnp.maximum(number, 1.0)
        high = shift.astype(BF16).astype(F32)
        middle = (shift - high).astype(BF16).astype(F32)
        low = (shift - high - middle).astype(BF16).astype(F32)
        shift = high + middle + low
        rest = jnp.where(live, kept - shift, 0.0)
        carried = jnp.where(row == 0, high, jnp.where(row == 1, middle, jnp.where(row == 2, low, 0.0)))
        blocks = [rest[i : i + QUAD] for i in range(0, days, QUAD)] + [carried]
        for i, block in enumerate(blocks):
            block = block.astype(BF16)
            for j in range(parts):
                out_ref[w * parts + j, :, i * LANES : (i + 1) * LANES] = block[:, j * LANES : (j + 1) * LANES]


def scale_kernel(got_ref, starts_ref, block_ref, out_ref):
    sources = got_ref.shape[0]
    days = (got_ref.shape[2] // LANES - 1) * QUAD
    total = sources * days
    parts = sources // starts_ref.shape[0]
    w = lax.axis_index("window")
    own = pl.ds(pl.multiple_of(lax.axis_index(ROWS) % parts * LANES, LANES), LANES)
    starts = starts_ref[:, own]
    starts = jnp.sum(jnp.where(lax.broadcasted_iota(jnp.int32, starts.shape, 0) == w, starts, 0), axis=0, keepdims=True)
    got = got_ref[...].astype(F32)
    lanes = [got[:, :, at : at + LANES] for at in range(0, got.shape[2], LANES)]
    shift = jnp.sum(lanes[-1], axis=1, keepdims=True)
    eights = [jnp.concatenate(lanes[i : i + 2], axis=1) + shift for i in range(0, len(lanes) - 1, 2)]
    values = jnp.concatenate([eight.reshape(sources * EIGHT, LANES) for eight in eights], axis=0)
    row = lax.broadcasted_iota(jnp.int32, (total, LANES), 0)
    eight, source = row // (sources * EIGHT), row % (sources * EIGHT) // EIGHT
    live = source * days + eight * EIGHT + row % EIGHT >= starts
    counts = (total - starts).astype(F32)
    mean = jnp.sum(jnp.where(live, values, 0.0), axis=0, keepdims=True) / counts
    centered = jnp.where(live, values - mean, 0.0)
    squares = jnp.sum(centered * centered, axis=0, keepdims=True)
    scaled = centered * lax.rsqrt(squares + 1.0)
    out_ref[0:total, :] = scaled
    out_ref[total:, :] = block_ref[w, :, own].astype(BF16).astype(F32)


def gram_kernel(both_ref, out_ref, all_ref):
    cores, rows, _ = both_ref.shape
    total = rows // LANES * LANES
    both = jnp.concatenate([both_ref[c] for c in range(cores)], axis=1)
    high, low = split(both[:total])
    rounded = both[total:].astype(BF16)
    blocks = total // LANES
    across = ((1,), (1,))
    proj = dot(rounded, high, across, None) + dot(rounded, low, across, None)
    rest = []
    at = 0

    def put(tile):
        nonlocal at
        all_ref[at : at + tile.shape[0], :] = tile
        at += tile.shape[0]

    for a in range(blocks):
        here, on = slice(a * LANES, (a + 1) * LANES), slice(a * LANES, total)
        strip = dot(high[here], high[on], across, None)
        strip += dot(low[here], high[on], across, None) + dot(high[here], low[on], across, None)
        put(strip[:HALF, :LANES])
        rest.append(strip[HALF:, :LANES])
        for b in range(1, blocks - a):
            put(strip[:, b * LANES : (b + 1) * LANES])
    left = lax.broadcasted_iota(jnp.int32, (HALF, LANES), 1) < HALF
    for a in range(0, blocks, 2):
        put(jnp.where(left, pltpu.roll(rest[a], HALF, 1), rest[a + 1]))
    for b in range(blocks):
        put(proj[:, b * LANES : (b + 1) * LANES])
    if at < all_ref.shape[0]:
        all_ref[at:, :] = jnp.zeros((all_ref.shape[0] - at, LANES), F32)
    share = out_ref.shape[0]
    out_ref[...] = all_ref[pl.ds(pl.multiple_of(lax.axis_index("sub") * share, EIGHT), share), :]


def inverse_lower(gram):
    k = gram.shape[0]
    size = 8
    row = lax.broadcasted_iota(jnp.int32, (k, LANES), 0)
    lane = lax.broadcasted_iota(jnp.int32, (k, LANES), 1)
    both = jnp.concatenate([gram, jnp.zeros((k, LANES - k), F32)], axis=1)
    both = jnp.where(lane == row + k, 1.0, both)
    for i in range(0, k, size):
        columns = [jnp.broadcast_to(both[:, i + q : i + q + 1], (k, LANES)) for q in range(size)]
        lines = [both[i + q : i + q + 1, :] for q in range(size)]
        inner = {(q, p): columns[q][i + p : i + p + 1, :] for q in range(size) for p in range(q, size)}
        update = jnp.zeros((k, LANES), F32)
        for q in range(size):
            inverse = 1.0 / inner[q, q]
            later = range(q + 1, size)
            ratio = {p: inner[q, p] * inverse for p in later}
            for p in later:
                for r in range(p, size):
                    inner[p, r] -= ratio[p] * inner[q, r]
            for p in later:
                lines[p] -= ratio[p] * lines[q]
                columns[p] -= columns[q] * ratio[p]
            update += jnp.where(row > i + q, columns[q] * inverse, 0.0) * lines[q]
        both -= update
    pivots = jnp.sum(jnp.where(lane == row, both, 0.0), axis=1, keepdims=True)
    return (both * lax.rsqrt(pivots))[:, k : 2 * k]


def iterate_kernel(assets, got_ref, scaled_ref, out_ref, high_ref, low_ref):
    factors = out_ref.shape[1]
    total = scaled_ref.shape[0] - factors
    blocks = total // LANES
    row = lax.broadcasted_iota(jnp.int32, (LANES, LANES), 0)
    lane = lax.broadcasted_iota(jnp.int32, (LANES, LANES), 1)
    at = 0

    def take(rows):
        nonlocal at
        at += rows
        return got_ref[at - rows : at, :]

    tops = []
    for a in range(blocks):
        here = slice(a * LANES, (a + 1) * LANES)
        tops.append(take(HALF))
        for b in range(a + 1, blocks):
            there = slice(b * LANES, (b + 1) * LANES)
            tile = take(LANES)
            high_ref[here, there], low_ref[here, there] = split(tile)
            high_ref[there, here], low_ref[there, here] = split(tile.T)
    for a in range(0, blocks, 2):
        pair = take(HALF)
        for c, rest in ((a, pltpu.roll(pair, HALF, 1)), (a + 1, pair)):
            here = slice(c * LANES, (c + 1) * LANES)
            tile = jnp.concatenate([tops[c], rest], axis=0)
            tile = jnp.where((row >= HALF) & (lane < HALF), tile.T, tile)
            high_ref[here, here], low_ref[here, here] = split(tile)
    proj = jnp.concatenate([take(factors) for b in range(blocks)], axis=1)
    inward = ((1,), (0,))
    for step in range(ITERS):
        high, low = split(proj)
        stacked = dot(jnp.concatenate([high, low], axis=0), high_ref[...], inward, None)
        moved = stacked[:factors] + (stacked[factors:] + dot(high, low_ref[...], inward, None))
        gram = dot(moved, proj, ((1,), (1,))) * (1.0 / assets)
        proj = dot(inverse_lower(gram), moved if step < ITERS - 1 else proj, inward)
    loadings = dot3(proj, scaled_ref[0:total, :], inward).astype(BF16)
    out_ref[...] = jnp.broadcast_to(loadings[None], out_ref.shape)


def unpack_kernel(got_ref, out_ref):
    windows, _, width = out_ref.shape
    near, blocks = got_ref.shape[:2]
    for w in range(windows):
        for j in range(width // LANES):
            block = w * (blocks // windows) + j // near
            out_ref[w, :, j * LANES : (j + 1) * LANES] = got_ref[j % near, block].astype(F32)


def on_device(returns, starts, start_block):
    windows, days, width = returns.shape
    factors = start_block.shape[1]
    parts = width // LANES
    rows = windows * parts
    cols, sub = lax.axis_size("cols"), lax.axis_size("sub")
    sides = cols * sub
    total = days * rows
    assets = width * sides
    quad, block = ("mid", "near"), ("near", "cols")

    packed = pl.pallas_call(
        pack_kernel,
        out_shape=jax.ShapeDtypeStruct((rows, QUAD, (days // QUAD + 1) * LANES), BF16),
        in_specs=[VMEM, VMEM],
        out_specs=VMEM,
        name="pack",
    )(returns, starts)
    got = lax.all_to_all(packed, ROWS, 0, 0, tiled=True)

    blocks = total // LANES
    filled = blocks * (blocks - 1) // 2 * LANES + blocks // 2 * 3 * HALF + factors * blocks
    unit = EIGHT * sub * lax.axis_size(block)
    height = (filled + unit - 1) // unit * unit
    scaled = pl.pallas_call(
        scale_kernel,
        out_shape=jax.ShapeDtypeStruct((total + factors, LANES), F32),
        in_specs=[VMEM, VMEM, VMEM],
        out_specs=VMEM,
        compiler_params=PARAMS,
        name="scale",
    )(got, starts, start_block)
    both = lax.all_gather(scaled, "sub")
    partial = pl.pallas_call(
        gram_kernel,
        out_shape=jax.ShapeDtypeStruct((height // sub, LANES), F32),
        in_specs=[VMEM],
        out_specs=VMEM,
        scratch_shapes=[pltpu.VMEM((height, LANES), F32)],
        compiler_params=PARAMS,
        name="gram",
    )(both)

    pieces = lax.axis_size(block)
    share = height // sub // pieces
    own = lax.all_to_all(partial.reshape(pieces, share, LANES), block, 0, 0, tiled=True).sum(axis=0)
    own = lax.all_gather(own, "mid").sum(axis=0)
    own = lax.all_gather(own, "far").sum(axis=0)
    own = lax.all_to_all(jnp.broadcast_to(own[None], (pieces, share, LANES)), block, 0, 0, tiled=True)
    whole = lax.all_gather(own.reshape(height // sub, LANES), "sub", tiled=True)

    far = windows * parts // NEAR
    sent = pl.pallas_call(
        functools.partial(iterate_kernel, assets),
        out_shape=jax.ShapeDtypeStruct((far, factors, LANES), BF16),
        in_specs=[VMEM, VMEM],
        out_specs=VMEM,
        scratch_shapes=[pltpu.VMEM((total, total), BF16)] * 2,
        compiler_params=PARAMS,
        name="iterate",
    )(whole, scaled)
    got = lax.all_to_all(sent, ("window", "far"), 0, 0, tiled=True)
    got = lax.all_to_all(jnp.broadcast_to(got[None], (NEAR, *got.shape)), quad, 0, 0, tiled=True)
    return pl.pallas_call(
        unpack_kernel,
        out_shape=jax.ShapeDtypeStruct((windows, factors, width), F32),
        in_specs=[VMEM],
        out_specs=VMEM,
        compiler_params=PARAMS,
        name="unpack",
    )(got)


def solution(mesh):
    groups, rows, cols, sub = (mesh.shape[name] for name in ("groups", "rows", "cols", "sub"))

    def whole(returns, starts, start_block):
        windows = returns.shape[0] // groups
        split = Mesh(
            mesh.devices.reshape(groups, windows, rows // windows // NEAR, NEAR // 2, 2, cols, sub),
            ("groups", "window", "far", "mid", "near", "cols", "sub"),
        )
        placed = (
            P("groups", ("window", "far", "mid", "near"), ("cols", "sub")),
            P("groups", ("cols", "sub")),
            P("groups", None, ("cols", "sub")),
        )
        return jax.shard_map(
            on_device,
            mesh=split,
            in_specs=placed,
            out_specs=P("groups", None, ("cols", "sub")),
            check_vma=False,
        )(returns, starts, start_block)

    return whole
```

```python
import functools

import jax
import jax.numpy as jnp
from jax import lax
from jax.experimental import pallas as pl
from jax.experimental.pallas import tpu as pltpu
from jax.sharding import Mesh
from jax.sharding import PartitionSpec as P

ITERS = 3
LANES = 128
ROWS = ("window", "far", "mid", "near")
HALF = LANES // 2
NEAR = 4
EIGHT = 8
QUAD = 4
F32 = jnp.float32
BF16 = jnp.bfloat16
HIGHEST = lax.Precision.HIGHEST
VMEM = pl.BlockSpec(memory_space=pltpu.VMEM)
PARAMS = pltpu.CompilerParams(vmem_limit_bytes=16 << 20)


def dot(a, b, dims, precision=HIGHEST):
    return lax.dot_general(a, b, (dims, ((), ())), precision=precision, preferred_element_type=F32)


def split(a):
    high = a.astype(BF16)
    return high, (a - high.astype(F32)).astype(BF16)


def dot3(a, b, dims):
    (ah, al), (bh, bl) = split(a), split(b)
    return dot(ah, bh, dims, None) + (dot(al, bh, dims, None) + dot(ah, bl, dims, None))


def pack_kernel(returns_ref, starts_ref, out_ref):
    windows, days, width = returns_ref.shape
    parts = width // LANES
    day = lax.broadcasted_iota(jnp.int32, (days, width), 0) + lax.axis_index(ROWS) * days
    row = lax.broadcasted_iota(jnp.int32, (QUAD, width), 0)
    for w in range(windows):
        live = day >= starts_ref[w : w + 1, :]
        kept = jnp.where(live, returns_ref[w], 0.0)
        number = jnp.sum(live.astype(F32), axis=0, keepdims=True)
        shift = jnp.sum(kept, axis=0, keepdims=True) / jnp.maximum(number, 1.0)
        high = shift.astype(BF16).astype(F32)
        middle = (shift - high).astype(BF16).astype(F32)
        low = (shift - high - middle).astype(BF16).astype(F32)
        shift = high + middle + low
        rest = jnp.where(live, kept - shift, 0.0)
        carried = jnp.where(row == 0, high, jnp.where(row == 1, middle, jnp.where(row == 2, low, 0.0)))
        blocks = [rest[i : i + QUAD] for i in range(0, days, QUAD)] + [carried]
        for i, block in enumerate(blocks):
            block = block.astype(BF16)
            for j in range(parts):
                out_ref[w * parts + j, :, i * LANES : (i + 1) * LANES] = block[:, j * LANES : (j + 1) * LANES]


def scale_kernel(got_ref, starts_ref, block_ref, out_ref):
    sources = got_ref.shape[0]
    days = (got_ref.shape[2] // LANES - 1) * QUAD
    total = sources * days
    parts = sources // starts_ref.shape[0]
    w = lax.axis_index("window")
    own = pl.ds(pl.multiple_of(lax.axis_index(ROWS) % parts * LANES, LANES), LANES)
    starts = starts_ref[:, own]
    starts = jnp.sum(jnp.where(lax.broadcasted_iota(jnp.int32, starts.shape, 0) == w, starts, 0), axis=0, keepdims=True)
    got = got_ref[...].astype(F32)
    lanes = [got[:, :, at : at + LANES] for at in range(0, got.shape[2], LANES)]
    shift = jnp.sum(lanes[-1], axis=1, keepdims=True)
    eights = [jnp.concatenate(lanes[i : i + 2], axis=1) + shift for i in range(0, len(lanes) - 1, 2)]
    values = jnp.concatenate([eight.reshape(sources * EIGHT, LANES) for eight in eights], axis=0)
    row = lax.broadcasted_iota(jnp.int32, (total, LANES), 0)
    eight, source = row // (sources * EIGHT), row % (sources * EIGHT) // EIGHT
    live = source * days + eight * EIGHT + row % EIGHT >= starts
    counts = (total - starts).astype(F32)
    mean = jnp.sum(jnp.where(live, values, 0.0), axis=0, keepdims=True) / counts
    centered = jnp.where(live, values - mean, 0.0)
    squares = jnp.sum(centered * centered, axis=0, keepdims=True)
    scaled = centered * lax.rsqrt(squares + 1.0)
    out_ref[0:total, :] = scaled
    out_ref[total:, :] = block_ref[w, :, own].astype(BF16).astype(F32)


def gram_kernel(both_ref, out_ref, all_ref):
    cores, rows, _ = both_ref.shape
    total = rows // LANES * LANES
    both = jnp.concatenate([both_ref[c] for c in range(cores)], axis=1)
    high, low = split(both[:total])
    rounded = both[total:].astype(BF16)
    blocks = total // LANES
    across = ((1,), (1,))
    proj = dot(rounded, high, across, None) + dot(rounded, low, across, None)
    rest = []
    at = 0

    def put(tile):
        nonlocal at
        all_ref[at : at + tile.shape[0], :] = tile
        at += tile.shape[0]

    for a in range(blocks):
        here, on = slice(a * LANES, (a + 1) * LANES), slice(a * LANES, total)
        strip = dot(high[here], high[on], across, None)
        strip += dot(low[here], high[on], across, None) + dot(high[here], low[on], across, None)
        put(strip[:HALF, :LANES])
        rest.append(strip[HALF:, :LANES])
        for b in range(1, blocks - a):
            put(strip[:, b * LANES : (b + 1) * LANES])
    left = lax.broadcasted_iota(jnp.int32, (HALF, LANES), 1) < HALF
    for a in range(0, blocks, 2):
        put(jnp.where(left, pltpu.roll(rest[a], HALF, 1), rest[a + 1]))
    for b in range(blocks):
        put(proj[:, b * LANES : (b + 1) * LANES])
    if at < all_ref.shape[0]:
        all_ref[at:, :] = jnp.zeros((all_ref.shape[0] - at, LANES), F32)
    share = out_ref.shape[0]
    out_ref[...] = all_ref[pl.ds(pl.multiple_of(lax.axis_index("sub") * share, EIGHT), share), :]


def inverse_lower(gram):
    k = gram.shape[0]
    size = 8
    row = lax.broadcasted_iota(jnp.int32, (k, LANES), 0)
    lane = lax.broadcasted_iota(jnp.int32, (k, LANES), 1)
    both = jnp.concatenate([gram, jnp.zeros((k, LANES - k), F32)], axis=1)
    both = jnp.where(lane == row + k, 1.0, both)
    for i in range(0, k, size):
        columns = [jnp.broadcast_to(both[:, i + q : i + q + 1], (k, LANES)) for q in range(size)]
        lines = [both[i + q : i + q + 1, :] for q in range(size)]
        inner = {(q, p): columns[q][i + p : i + p + 1, :] for q in range(size) for p in range(q, size)}
        update = jnp.zeros((k, LANES), F32)
        for q in range(size):
            inverse = 1.0 / inner[q, q]
            later = range(q + 1, size)
            ratio = {p: inner[q, p] * inverse for p in later}
            for p in later:
                for r in range(p, size):
                    inner[p, r] -= ratio[p] * inner[q, r]
            for p in later:
                lines[p] -= ratio[p] * lines[q]
                columns[p] -= columns[q] * ratio[p]
            update += jnp.where(row > i + q, columns[q] * inverse, 0.0) * lines[q]
        both -= update
    pivots = jnp.sum(jnp.where(lane == row, both, 0.0), axis=1, keepdims=True)
    return (both * lax.rsqrt(pivots))[:, k : 2 * k]


def iterate_kernel(assets, got_ref, scaled_ref, out_ref, high_ref, low_ref):
    factors = out_ref.shape[1]
    total = scaled_ref.shape[0] - factors
    blocks = total // LANES
    row = lax.broadcasted_iota(jnp.int32, (LANES, LANES), 0)
    lane = lax.broadcasted_iota(jnp.int32, (LANES, LANES), 1)
    at = 0

    def take(rows):
        nonlocal at
        at += rows
        return got_ref[at - rows : at, :]

    tops = []
    for a in range(blocks):
        here = slice(a * LANES, (a + 1) * LANES)
        tops.append(take(HALF))
        for b in range(a + 1, blocks):
            there = slice(b * LANES, (b + 1) * LANES)
            tile = take(LANES)
            high_ref[here, there], low_ref[here, there] = split(tile)
            high_ref[there, here], low_ref[there, here] = split(tile.T)
    for a in range(0, blocks, 2):
        pair = take(HALF)
        for c, rest in ((a, pltpu.roll(pair, HALF, 1)), (a + 1, pair)):
            here = slice(c * LANES, (c + 1) * LANES)
            tile = jnp.concatenate([tops[c], rest], axis=0)
            tile = jnp.where((row >= HALF) & (lane < HALF), tile.T, tile)
            high_ref[here, here], low_ref[here, here] = split(tile)
    proj = jnp.concatenate([take(factors) for b in range(blocks)], axis=1)
    inward = ((1,), (0,))
    for step in range(ITERS):
        high, low = split(proj)
        stacked = dot(jnp.concatenate([high, low], axis=0), high_ref[...], inward, None)
        moved = stacked[:factors] + (stacked[factors:] + dot(high, low_ref[...], inward, None))
        gram = dot(moved, proj, ((1,), (1,))) * (1.0 / assets)
        proj = dot(inverse_lower(gram), moved if step < ITERS - 1 else proj, inward)
    loadings = dot3(proj, scaled_ref[0:total, :], inward).astype(BF16)
    out_ref[...] = jnp.broadcast_to(loadings[None], out_ref.shape)


def unpack_kernel(got_ref, out_ref):
    windows, _, width = out_ref.shape
    near, blocks = got_ref.shape[:2]
    for w in range(windows):
        for j in range(width // LANES):
            block = w * (blocks // windows) + j // near
            out_ref[w, :, j * LANES : (j + 1) * LANES] = got_ref[j % near, block].astype(F32)


def on_device(returns, starts, start_block):
    windows, days, width = returns.shape
    factors = start_block.shape[1]
    parts = width // LANES
    rows = windows * parts
    cols, sub = lax.axis_size("cols"), lax.axis_size("sub")
    sides = cols * sub
    total = days * rows
    assets = width * sides
    quad, block = ("mid", "near"), ("near", "cols")

    packed = pl.pallas_call(
        pack_kernel,
        out_shape=jax.ShapeDtypeStruct((rows, QUAD, (days // QUAD + 1) * LANES), BF16),
        in_specs=[VMEM, VMEM],
        out_specs=VMEM,
        name="pack",
    )(returns, starts)
    got = lax.all_to_all(packed, ROWS, 0, 0, tiled=True)

    blocks = total // LANES
    filled = blocks * (blocks - 1) // 2 * LANES + blocks // 2 * 3 * HALF + factors * blocks
    unit = EIGHT * sub * lax.axis_size(block)
    height = (filled + unit - 1) // unit * unit
    scaled = pl.pallas_call(
        scale_kernel,
        out_shape=jax.ShapeDtypeStruct((total + factors, LANES), F32),
        in_specs=[VMEM, VMEM, VMEM],
        out_specs=VMEM,
        compiler_params=PARAMS,
        name="scale",
    )(got, starts, start_block)
    both = lax.all_gather(scaled, "sub")
    partial = pl.pallas_call(
        gram_kernel,
        out_shape=jax.ShapeDtypeStruct((height // sub, LANES), F32),
        in_specs=[VMEM],
        out_specs=VMEM,
        scratch_shapes=[pltpu.VMEM((height, LANES), F32)],
        compiler_params=PARAMS,
        name="gram",
    )(both)

    pieces = lax.axis_size(block)
    share = height // sub // pieces
    own = lax.all_to_all(partial.reshape(pieces, share, LANES), block, 0, 0, tiled=True).sum(axis=0)
    even = ("far", "mid")
    own = lax.all_to_all(jnp.broadcast_to(own[None], (lax.axis_size(even), share, LANES)), even, 0, 0, tiled=True).sum(axis=0)
    own = lax.all_to_all(jnp.broadcast_to(own[None], (pieces, share, LANES)), block, 0, 0, tiled=True)
    whole = lax.all_gather(own.reshape(height // sub, LANES), "sub", tiled=True)

    far = windows * parts // NEAR
    sent = pl.pallas_call(
        functools.partial(iterate_kernel, assets),
        out_shape=jax.ShapeDtypeStruct((far, factors, LANES), BF16),
        in_specs=[VMEM, VMEM],
        out_specs=VMEM,
        scratch_shapes=[pltpu.VMEM((total, total), BF16)] * 2,
        compiler_params=PARAMS,
        name="iterate",
    )(whole, scaled)
    got = lax.all_to_all(sent, ("window", "far"), 0, 0, tiled=True)
    got = lax.all_to_all(jnp.broadcast_to(got[None], (NEAR, *got.shape)), quad, 0, 0, tiled=True)
    return pl.pallas_call(
        unpack_kernel,
        out_shape=jax.ShapeDtypeStruct((windows, factors, width), F32),
        in_specs=[VMEM],
        out_specs=VMEM,
        compiler_params=PARAMS,
        name="unpack",
    )(got)


def solution(mesh):
    groups, rows, cols, sub = (mesh.shape[name] for name in ("groups", "rows", "cols", "sub"))

    def whole(returns, starts, start_block):
        windows = returns.shape[0] // groups
        split = Mesh(
            mesh.devices.reshape(groups, windows, rows // windows // NEAR, NEAR // 2, 2, cols, sub),
            ("groups", "window", "far", "mid", "near", "cols", "sub"),
        )
        placed = (
            P("groups", ("window", "far", "mid", "near"), ("cols", "sub")),
            P("groups", ("cols", "sub")),
            P("groups", None, ("cols", "sub")),
        )
        return jax.shard_map(
            on_device,
            mesh=split,
            in_specs=placed,
            out_specs=P("groups", None, ("cols", "sub")),
            check_vma=False,
        )(returns, starts, start_block)

    return whole
```

```python
import functools

import jax
import jax.numpy as jnp
from jax import lax
from jax.experimental import pallas as pl
from jax.experimental.pallas import tpu as pltpu
from jax.sharding import Mesh
from jax.sharding import PartitionSpec as P

ITERS = 3
LANES = 128
ROWS = ("window", "far", "mid", "near")
HALF = LANES // 2
NEAR = 4
EIGHT = 8
QUAD = 4
F32 = jnp.float32
BF16 = jnp.bfloat16
HIGHEST = lax.Precision.HIGHEST
VMEM = pl.BlockSpec(memory_space=pltpu.VMEM)
PARAMS = pltpu.CompilerParams(vmem_limit_bytes=16 << 20)


def dot(a, b, dims, precision=HIGHEST):
    return lax.dot_general(a, b, (dims, ((), ())), precision=precision, preferred_element_type=F32)


def split(a):
    high = a.astype(BF16)
    return high, (a - high.astype(F32)).astype(BF16)


def pack_kernel(returns_ref, starts_ref, out_ref):
    windows, days, width = returns_ref.shape
    parts = width // LANES
    day = lax.broadcasted_iota(jnp.int32, (days, width), 0) + lax.axis_index(ROWS) * days
    row = lax.broadcasted_iota(jnp.int32, (QUAD, width), 0)
    for w in range(windows):
        live = day >= starts_ref[w : w + 1, :]
        kept = jnp.where(live, returns_ref[w], 0.0)
        number = jnp.sum(live.astype(F32), axis=0, keepdims=True)
        shift = jnp.sum(kept, axis=0, keepdims=True) / jnp.maximum(number, 1.0)
        high = shift.astype(BF16).astype(F32)
        middle = (shift - high).astype(BF16).astype(F32)
        low = (shift - high - middle).astype(BF16).astype(F32)
        shift = high + middle + low
        rest = jnp.where(live, kept - shift, 0.0)
        carried = jnp.where(row == 0, high, jnp.where(row == 1, middle, jnp.where(row == 2, low, 0.0)))
        blocks = [rest[i : i + QUAD] for i in range(0, days, QUAD)] + [carried]
        for i, block in enumerate(blocks):
            block = block.astype(BF16)
            for j in range(parts):
                out_ref[w * parts + j, :, i * LANES : (i + 1) * LANES] = block[:, j * LANES : (j + 1) * LANES]


def scale_kernel(got_ref, starts_ref, block_ref, out_ref):
    sources = got_ref.shape[0]
    days = (got_ref.shape[2] // LANES - 1) * QUAD
    total = sources * days
    parts = sources // starts_ref.shape[0]
    w = lax.axis_index("window")
    own = pl.ds(pl.multiple_of(lax.axis_index(ROWS) % parts * LANES, LANES), LANES)
    starts = starts_ref[:, own]
    starts = jnp.sum(jnp.where(lax.broadcasted_iota(jnp.int32, starts.shape, 0) == w, starts, 0), axis=0, keepdims=True)
    got = got_ref[...].astype(F32)
    lanes = [got[:, :, at : at + LANES] for at in range(0, got.shape[2], LANES)]
    shift = jnp.sum(lanes[-1], axis=1, keepdims=True)
    eights = [jnp.concatenate(lanes[i : i + 2], axis=1) + shift for i in range(0, len(lanes) - 1, 2)]
    values = jnp.concatenate([eight.reshape(sources * EIGHT, LANES) for eight in eights], axis=0)
    row = lax.broadcasted_iota(jnp.int32, (total, LANES), 0)
    eight, source = row // (sources * EIGHT), row % (sources * EIGHT) // EIGHT
    live = source * days + eight * EIGHT + row % EIGHT >= starts
    counts = (total - starts).astype(F32)
    mean = jnp.sum(jnp.where(live, values, 0.0), axis=0, keepdims=True) / counts
    centered = jnp.where(live, values - mean, 0.0)
    squares = jnp.sum(centered * centered, axis=0, keepdims=True)
    scaled = centered * lax.rsqrt(squares + 1.0)
    out_ref[0:total, :] = scaled.astype(BF16)
    out_ref[total:, :] = block_ref[w, :, own].astype(BF16)


def gram_kernel(both_ref, out_ref, all_ref):
    cores, rows, _ = both_ref.shape
    total = rows // LANES * LANES
    both = jnp.concatenate([both_ref[c] for c in range(cores)], axis=1)
    scaled, rounded = both[:total], both[total:]
    blocks = total // LANES
    across = ((1,), (1,))
    proj = dot(rounded, scaled, across, None)
    rest = []
    at = 0

    def put(tile):
        nonlocal at
        all_ref[at : at + tile.shape[0], :] = tile
        at += tile.shape[0]

    for a in range(blocks):
        here, on = slice(a * LANES, (a + 1) * LANES), slice(a * LANES, total)
        strip = dot(scaled[here], scaled[on], across, None)
        put(strip[:HALF, :LANES])
        rest.append(strip[HALF:, :LANES])
        for b in range(1, blocks - a):
            put(strip[:, b * LANES : (b + 1) * LANES])
    left = lax.broadcasted_iota(jnp.int32, (HALF, LANES), 1) < HALF
    for a in range(0, blocks, 2):
        put(jnp.where(left, pltpu.roll(rest[a], HALF, 1), rest[a + 1]))
    for b in range(blocks):
        put(proj[:, b * LANES : (b + 1) * LANES])
    if at < all_ref.shape[0]:
        all_ref[at:, :] = jnp.zeros((all_ref.shape[0] - at, LANES), F32)
    share = out_ref.shape[0]
    out_ref[...] = all_ref[pl.ds(pl.multiple_of(lax.axis_index("sub") * share, EIGHT), share), :]


def inverse_lower(gram):
    k = gram.shape[0]
    size = 8
    row = lax.broadcasted_iota(jnp.int32, (k, LANES), 0)
    lane = lax.broadcasted_iota(jnp.int32, (k, LANES), 1)
    both = jnp.concatenate([gram, jnp.zeros((k, LANES - k), F32)], axis=1)
    both = jnp.where(lane == row + k, 1.0, both)
    for i in range(0, k, size):
        columns = [jnp.broadcast_to(both[:, i + q : i + q + 1], (k, LANES)) for q in range(size)]
        lines = [both[i + q : i + q + 1, :] for q in range(size)]
        inner = {(q, p): columns[q][i + p : i + p + 1, :] for q in range(size) for p in range(q, size)}
        update = jnp.zeros((k, LANES), F32)
        for q in range(size):
            inverse = 1.0 / inner[q, q]
            later = range(q + 1, size)
            ratio = {p: inner[q, p] * inverse for p in later}
            for p in later:
                for r in range(p, size):
                    inner[p, r] -= ratio[p] * inner[q, r]
            for p in later:
                lines[p] -= ratio[p] * lines[q]
                columns[p] -= columns[q] * ratio[p]
            update += jnp.where(row > i + q, columns[q] * inverse, 0.0) * lines[q]
        both -= update
    pivots = jnp.sum(jnp.where(lane == row, both, 0.0), axis=1, keepdims=True)
    return (both * lax.rsqrt(pivots))[:, k : 2 * k]


def iterate_kernel(assets, got_ref, scaled_ref, out_ref, high_ref, low_ref):
    factors = out_ref.shape[1]
    total = scaled_ref.shape[0] - factors
    blocks = total // LANES
    row = lax.broadcasted_iota(jnp.int32, (LANES, LANES), 0)
    lane = lax.broadcasted_iota(jnp.int32, (LANES, LANES), 1)
    at = 0

    def take(rows):
        nonlocal at
        at += rows
        return got_ref[at - rows : at, :]

    tops = []
    for a in range(blocks):
        here = slice(a * LANES, (a + 1) * LANES)
        tops.append(take(HALF))
        for b in range(a + 1, blocks):
            there = slice(b * LANES, (b + 1) * LANES)
            tile = take(LANES)
            high_ref[here, there], low_ref[here, there] = split(tile)
            high_ref[there, here], low_ref[there, here] = split(tile.T)
    for a in range(0, blocks, 2):
        pair = take(HALF)
        for c, rest in ((a, pltpu.roll(pair, HALF, 1)), (a + 1, pair)):
            here = slice(c * LANES, (c + 1) * LANES)
            tile = jnp.concatenate([tops[c], rest], axis=0)
            tile = jnp.where((row >= HALF) & (lane < HALF), tile.T, tile)
            high_ref[here, here], low_ref[here, here] = split(tile)
    proj = jnp.concatenate([take(factors) for b in range(blocks)], axis=1)
    inward = ((1,), (0,))
    for step in range(ITERS):
        high, low = split(proj)
        stacked = dot(jnp.concatenate([high, low], axis=0), high_ref[...], inward, None)
        moved = stacked[:factors] + (stacked[factors:] + dot(high, low_ref[...], inward, None))
        gram = dot(moved, proj, ((1,), (1,))) * (1.0 / assets)
        proj = dot(inverse_lower(gram), moved if step < ITERS - 1 else proj, inward)
    high, low = split(proj)
    scaled = scaled_ref[0:total, :]
    loadings = (dot(high, scaled, inward, None) + dot(low, scaled, inward, None)).astype(BF16)
    out_ref[...] = jnp.broadcast_to(loadings[None], out_ref.shape)


def unpack_kernel(got_ref, out_ref):
    windows, _, width = out_ref.shape
    near, blocks = got_ref.shape[:2]
    for w in range(windows):
        for j in range(width // LANES):
            block = w * (blocks // windows) + j // near
            out_ref[w, :, j * LANES : (j + 1) * LANES] = got_ref[j % near, block].astype(F32)


def on_device(returns, starts, start_block):
    windows, days, width = returns.shape
    factors = start_block.shape[1]
    parts = width // LANES
    rows = windows * parts
    cols, sub = lax.axis_size("cols"), lax.axis_size("sub")
    sides = cols * sub
    total = days * rows
    assets = width * sides
    quad, block = ("mid", "near"), ("near", "cols")

    packed = pl.pallas_call(
        pack_kernel,
        out_shape=jax.ShapeDtypeStruct((rows, QUAD, (days // QUAD + 1) * LANES), BF16),
        in_specs=[VMEM, VMEM],
        out_specs=VMEM,
        name="pack",
    )(returns, starts)
    got = lax.all_to_all(packed, ROWS, 0, 0, tiled=True)

    blocks = total // LANES
    filled = blocks * (blocks - 1) // 2 * LANES + blocks // 2 * 3 * HALF + factors * blocks
    unit = EIGHT * sub * lax.axis_size(block)
    height = (filled + unit - 1) // unit * unit
    scaled = pl.pallas_call(
        scale_kernel,
        out_shape=jax.ShapeDtypeStruct((total + factors, LANES), BF16),
        in_specs=[VMEM, VMEM, VMEM],
        out_specs=VMEM,
        compiler_params=PARAMS,
        name="scale",
    )(got, starts, start_block)
    both = lax.all_gather(scaled, "sub")
    partial = pl.pallas_call(
        gram_kernel,
        out_shape=jax.ShapeDtypeStruct((height // sub, LANES), F32),
        in_specs=[VMEM],
        out_specs=VMEM,
        scratch_shapes=[pltpu.VMEM((height, LANES), F32)],
        compiler_params=PARAMS,
        name="gram",
    )(both)

    pieces = lax.axis_size(block)
    share = height // sub // pieces
    own = lax.all_to_all(partial.reshape(pieces, share, LANES), block, 0, 0, tiled=True).sum(axis=0)
    own = lax.all_gather(own, "mid").sum(axis=0)
    own = lax.all_gather(own, "far").sum(axis=0)
    own = lax.all_to_all(jnp.broadcast_to(own[None], (pieces, share, LANES)), block, 0, 0, tiled=True)
    whole = lax.all_gather(own.reshape(height // sub, LANES), "sub", tiled=True)

    far = windows * parts // NEAR
    sent = pl.pallas_call(
        functools.partial(iterate_kernel, assets),
        out_shape=jax.ShapeDtypeStruct((far, factors, LANES), BF16),
        in_specs=[VMEM, VMEM],
        out_specs=VMEM,
        scratch_shapes=[pltpu.VMEM((total, total), BF16)] * 2,
        compiler_params=PARAMS,
        name="iterate",
    )(whole, scaled)
    got = lax.all_to_all(sent, ("window", "far"), 0, 0, tiled=True)
    got = lax.all_to_all(jnp.broadcast_to(got[None], (NEAR, *got.shape)), quad, 0, 0, tiled=True)
    return pl.pallas_call(
        unpack_kernel,
        out_shape=jax.ShapeDtypeStruct((windows, factors, width), F32),
        in_specs=[VMEM],
        out_specs=VMEM,
        compiler_params=PARAMS,
        name="unpack",
    )(got)


def solution(mesh):
    groups, rows, cols, sub = (mesh.shape[name] for name in ("groups", "rows", "cols", "sub"))

    def whole(returns, starts, start_block):
        windows = returns.shape[0] // groups
        split = Mesh(
            mesh.devices.reshape(groups, windows, rows // windows // NEAR, NEAR // 2, 2, cols, sub),
            ("groups", "window", "far", "mid", "near", "cols", "sub"),
        )
        placed = (
            P("groups", ("window", "far", "mid", "near"), ("cols", "sub")),
            P("groups", ("cols", "sub")),
            P("groups", None, ("cols", "sub")),
        )
        return jax.shard_map(
            on_device,
            mesh=split,
            in_specs=placed,
            out_specs=P("groups", None, ("cols", "sub")),
            check_vma=False,
        )(returns, starts, start_block)

    return whole
```

```python
import functools

import jax
import jax.numpy as jnp
from jax import lax
from jax.experimental import pallas as pl
from jax.experimental.pallas import tpu as pltpu
from jax.sharding import Mesh
from jax.sharding import PartitionSpec as P

ITERS = 3
LANES = 128
ROWS = ("window", "far", "mid", "near")
HALF = LANES // 2
NEAR = 4
EIGHT = 8
QUAD = 4
F32 = jnp.float32
BF16 = jnp.bfloat16
HIGHEST = lax.Precision.HIGHEST
VMEM = pl.BlockSpec(memory_space=pltpu.VMEM)
PARAMS = pltpu.CompilerParams(vmem_limit_bytes=16 << 20)


def dot(a, b, dims, precision=HIGHEST):
    return lax.dot_general(a, b, (dims, ((), ())), precision=precision, preferred_element_type=F32)


def split(a):
    high = a.astype(BF16)
    return high, (a - high.astype(F32)).astype(BF16)


def pack_kernel(returns_ref, starts_ref, out_ref):
    windows, days, width = returns_ref.shape
    parts = width // LANES
    day = lax.broadcasted_iota(jnp.int32, (days, width), 0) + lax.axis_index(ROWS) * days
    row = lax.broadcasted_iota(jnp.int32, (QUAD, width), 0)
    for w in range(windows):
        live = day >= starts_ref[w : w + 1, :]
        kept = jnp.where(live, returns_ref[w], 0.0)
        number = jnp.sum(live.astype(F32), axis=0, keepdims=True)
        shift = jnp.sum(kept, axis=0, keepdims=True) / jnp.maximum(number, 1.0)
        high = shift.astype(BF16).astype(F32)
        middle = (shift - high).astype(BF16).astype(F32)
        low = (shift - high - middle).astype(BF16).astype(F32)
        shift = high + middle + low
        rest = jnp.where(live, kept - shift, 0.0)
        carried = jnp.where(row == 0, high, jnp.where(row == 1, middle, jnp.where(row == 2, low, 0.0)))
        blocks = [rest[i : i + QUAD] for i in range(0, days, QUAD)] + [carried]
        for i, block in enumerate(blocks):
            block = block.astype(BF16)
            for j in range(parts):
                out_ref[w * parts + j, :, i * LANES : (i + 1) * LANES] = block[:, j * LANES : (j + 1) * LANES]


def scale_kernel(got_ref, starts_ref, block_ref, out_ref):
    sources = got_ref.shape[0]
    days = (got_ref.shape[2] // LANES - 1) * QUAD
    total = sources * days
    parts = sources // starts_ref.shape[0]
    w = lax.axis_index("window")
    own = pl.ds(pl.multiple_of(lax.axis_index(ROWS) % parts * LANES, LANES), LANES)
    starts = starts_ref[:, own]
    starts = jnp.sum(jnp.where(lax.broadcasted_iota(jnp.int32, starts.shape, 0) == w, starts, 0), axis=0, keepdims=True)
    got = got_ref[...].astype(F32)
    lanes = [got[:, :, at : at + LANES] for at in range(0, got.shape[2], LANES)]
    shift = jnp.sum(lanes[-1], axis=1, keepdims=True)
    eights = [jnp.concatenate(lanes[i : i + 2], axis=1) + shift for i in range(0, len(lanes) - 1, 2)]
    values = jnp.concatenate([eight.reshape(sources * EIGHT, LANES) for eight in eights], axis=0)
    row = lax.broadcasted_iota(jnp.int32, (total, LANES), 0)
    eight, source = row // (sources * EIGHT), row % (sources * EIGHT) // EIGHT
    live = source * days + eight * EIGHT + row % EIGHT >= starts
    counts = (total - starts).astype(F32)
    mean = jnp.sum(jnp.where(live, values, 0.0), axis=0, keepdims=True) / counts
    centered = jnp.where(live, values - mean, 0.0)
    squares = jnp.sum(centered * centered, axis=0, keepdims=True)
    scaled = centered * lax.rsqrt(squares + 1.0)
    out_ref[0:total, :] = scaled.astype(BF16)
    out_ref[total:, :] = block_ref[w, :, own].astype(BF16)


def gram_kernel(both_ref, out_ref, all_ref):
    cores, rows, _ = both_ref.shape
    total = rows // LANES * LANES
    both = jnp.concatenate([both_ref[c] for c in range(cores)], axis=1)
    scaled, rounded = both[:total], both[total:]
    blocks = total // LANES
    across = ((1,), (1,))
    proj = dot(rounded, scaled, across, None)
    rest = []
    at = 0

    def put(tile):
        nonlocal at
        all_ref[at : at + tile.shape[0], :] = tile
        at += tile.shape[0]

    for a in range(blocks):
        here, on = slice(a * LANES, (a + 1) * LANES), slice(a * LANES, total)
        strip = dot(scaled[here], scaled[on], across, None)
        put(strip[:HALF, :LANES])
        rest.append(strip[HALF:, :LANES])
        for b in range(1, blocks - a):
            put(strip[:, b * LANES : (b + 1) * LANES])
    left = lax.broadcasted_iota(jnp.int32, (HALF, LANES), 1) < HALF
    for a in range(0, blocks, 2):
        put(jnp.where(left, pltpu.roll(rest[a], HALF, 1), rest[a + 1]))
    for b in range(blocks):
        put(proj[:, b * LANES : (b + 1) * LANES])
    if at < all_ref.shape[0]:
        all_ref[at:, :] = jnp.zeros((all_ref.shape[0] - at, LANES), F32)
    share = out_ref.shape[0]
    out_ref[...] = all_ref[pl.ds(pl.multiple_of(lax.axis_index("sub") * share, EIGHT), share), :]


def inverse_lower(gram):
    k = gram.shape[0]
    size = 8
    row = lax.broadcasted_iota(jnp.int32, (k, LANES), 0)
    lane = lax.broadcasted_iota(jnp.int32, (k, LANES), 1)
    both = jnp.concatenate([gram, jnp.zeros((k, LANES - k), F32)], axis=1)
    both = jnp.where(lane == row + k, 1.0, both)
    for i in range(0, k, size):
        columns = [jnp.broadcast_to(both[:, i + q : i + q + 1], (k, LANES)) for q in range(size)]
        lines = [both[i + q : i + q + 1, :] for q in range(size)]
        inner = {(q, p): columns[q][i + p : i + p + 1, :] for q in range(size) for p in range(q, size)}
        update = jnp.zeros((k, LANES), F32)
        for q in range(size):
            inverse = 1.0 / inner[q, q]
            later = range(q + 1, size)
            ratio = {p: inner[q, p] * inverse for p in later}
            for p in later:
                for r in range(p, size):
                    inner[p, r] -= ratio[p] * inner[q, r]
            for p in later:
                lines[p] -= ratio[p] * lines[q]
                columns[p] -= columns[q] * ratio[p]
            update += jnp.where(row > i + q, columns[q] * inverse, 0.0) * lines[q]
        both -= update
    pivots = jnp.sum(jnp.where(lane == row, both, 0.0), axis=1, keepdims=True)
    return (both * lax.rsqrt(pivots))[:, k : 2 * k]


def iterate_kernel(assets, got_ref, scaled_ref, out_ref, high_ref, low_ref):
    factors = out_ref.shape[1]
    total = scaled_ref.shape[0] - factors
    blocks = total // LANES
    row = lax.broadcasted_iota(jnp.int32, (LANES, LANES), 0)
    lane = lax.broadcasted_iota(jnp.int32, (LANES, LANES), 1)
    at = 0

    def take(rows):
        nonlocal at
        at += rows
        return got_ref[at - rows : at, :]

    tops = []
    for a in range(blocks):
        here = slice(a * LANES, (a + 1) * LANES)
        tops.append(take(HALF))
        for b in range(a + 1, blocks):
            there = slice(b * LANES, (b + 1) * LANES)
            tile = take(LANES)
            high_ref[here, there], low_ref[here, there] = split(tile)
            high_ref[there, here], low_ref[there, here] = split(tile.T)
    for a in range(0, blocks, 2):
        pair = take(HALF)
        for c, rest in ((a, pltpu.roll(pair, HALF, 1)), (a + 1, pair)):
            here = slice(c * LANES, (c + 1) * LANES)
            tile = jnp.concatenate([tops[c], rest], axis=0)
            tile = jnp.where((row >= HALF) & (lane < HALF), tile.T, tile)
            high_ref[here, here], low_ref[here, here] = split(tile)
    proj = jnp.concatenate([take(factors) for b in range(blocks)], axis=1)
    inward = ((1,), (0,))
    for step in range(ITERS):
        high, low = split(proj)
        stacked = dot(jnp.concatenate([high, low], axis=0), high_ref[...], inward, None)
        moved = stacked[:factors] + (stacked[factors:] + dot(high, low_ref[...], inward, None))
        gram = dot(moved, proj, ((1,), (1,))) * (1.0 / assets)
        proj = dot(inverse_lower(gram), moved if step < ITERS - 1 else proj, inward)
    high, low = split(proj)
    scaled = scaled_ref[0:total, :]
    loadings = (dot(high, scaled, inward, None) + dot(low, scaled, inward, None)).astype(BF16)
    out_ref[...] = jnp.broadcast_to(loadings[None], out_ref.shape)


def unpack_kernel(got_ref, out_ref):
    windows, _, width = out_ref.shape
    near, blocks = got_ref.shape[:2]
    for w in range(windows):
        for j in range(width // LANES):
            block = w * (blocks // windows) + j // near
            out_ref[w, :, j * LANES : (j + 1) * LANES] = got_ref[j % near, block].astype(F32)


def on_device(returns, starts, start_block):
    windows, days, width = returns.shape
    factors = start_block.shape[1]
    parts = width // LANES
    rows = windows * parts
    cols, sub = lax.axis_size("cols"), lax.axis_size("sub")
    sides = cols * sub
    total = days * rows
    assets = width * sides
    quad, block = ("mid", "near"), ("near", "cols")

    packed = pl.pallas_call(
        pack_kernel,
        out_shape=jax.ShapeDtypeStruct((rows, QUAD, (days // QUAD + 1) * LANES), BF16),
        in_specs=[VMEM, VMEM],
        out_specs=VMEM,
        name="pack",
    )(returns, starts)
    got = lax.all_to_all(packed, ROWS, 0, 0, tiled=True)

    blocks = total // LANES
    filled = blocks * (blocks - 1) // 2 * LANES + blocks // 2 * 3 * HALF + factors * blocks
    unit = EIGHT * sub * lax.axis_size(block)
    height = (filled + unit - 1) // unit * unit
    scaled = pl.pallas_call(
        scale_kernel,
        out_shape=jax.ShapeDtypeStruct((total + factors, LANES), BF16),
        in_specs=[VMEM, VMEM, VMEM],
        out_specs=VMEM,
        compiler_params=PARAMS,
        name="scale",
    )(got, starts, start_block)
    both = lax.all_gather(scaled, "sub")
    partial = pl.pallas_call(
        gram_kernel,
        out_shape=jax.ShapeDtypeStruct((height // sub, LANES), F32),
        in_specs=[VMEM],
        out_specs=VMEM,
        scratch_shapes=[pltpu.VMEM((height, LANES), F32)],
        compiler_params=PARAMS,
        name="gram",
    )(both)

    pieces = lax.axis_size(block)
    share = height // sub // pieces
    own = lax.all_to_all(partial.reshape(pieces, share, LANES), block, 0, 0, tiled=True).sum(axis=0)
    own = lax.all_gather(own, "far").sum(axis=0)
    own = lax.all_gather(own, "mid").sum(axis=0)
    own = lax.all_to_all(jnp.broadcast_to(own[None], (pieces, share, LANES)), block, 0, 0, tiled=True)
    whole = lax.all_gather(own.reshape(height // sub, LANES), "sub", tiled=True)

    far = windows * parts // NEAR
    sent = pl.pallas_call(
        functools.partial(iterate_kernel, assets),
        out_shape=jax.ShapeDtypeStruct((far, factors, LANES), BF16),
        in_specs=[VMEM, VMEM],
        out_specs=VMEM,
        scratch_shapes=[pltpu.VMEM((total, total), BF16)] * 2,
        compiler_params=PARAMS,
        name="iterate",
    )(whole, scaled)
    got = lax.all_to_all(sent, ("window", "far"), 0, 0, tiled=True)
    got = lax.all_to_all(jnp.broadcast_to(got[None], (NEAR, *got.shape)), quad, 0, 0, tiled=True)
    return pl.pallas_call(
        unpack_kernel,
        out_shape=jax.ShapeDtypeStruct((windows, factors, width), F32),
        in_specs=[VMEM],
        out_specs=VMEM,
        compiler_params=PARAMS,
        name="unpack",
    )(got)


def solution(mesh):
    groups, rows, cols, sub = (mesh.shape[name] for name in ("groups", "rows", "cols", "sub"))

    def whole(returns, starts, start_block):
        windows = returns.shape[0] // groups
        split = Mesh(
            mesh.devices.reshape(groups, windows, rows // windows // NEAR, NEAR // 2, 2, cols, sub),
            ("groups", "window", "far", "mid", "near", "cols", "sub"),
        )
        placed = (
            P("groups", ("window", "far", "mid", "near"), ("cols", "sub")),
            P("groups", ("cols", "sub")),
            P("groups", None, ("cols", "sub")),
        )
        return jax.shard_map(
            on_device,
            mesh=split,
            in_specs=placed,
            out_specs=P("groups", None, ("cols", "sub")),
            check_vma=False,
        )(returns, starts, start_block)

    return whole
```

```python
import functools

import jax
import jax.numpy as jnp
from jax import lax
from jax.experimental import pallas as pl
from jax.experimental.pallas import tpu as pltpu
from jax.sharding import Mesh
from jax.sharding import PartitionSpec as P

ITERS = 3
LANES = 128
ROWS = ("window", "far", "mid", "near")
HALF = LANES // 2
NEAR = 4
EIGHT = 8
QUAD = 4
F32 = jnp.float32
BF16 = jnp.bfloat16
HIGHEST = lax.Precision.HIGHEST
VMEM = pl.BlockSpec(memory_space=pltpu.VMEM)
PARAMS = pltpu.CompilerParams(vmem_limit_bytes=16 << 20)


def dot(a, b, dims, precision=HIGHEST):
    return lax.dot_general(a, b, (dims, ((), ())), precision=precision, preferred_element_type=F32)


def split(a):
    high = a.astype(BF16)
    return high, (a - high.astype(F32)).astype(BF16)


def pack_kernel(returns_ref, starts_ref, out_ref):
    windows, days, width = returns_ref.shape
    parts = width // LANES
    day = lax.broadcasted_iota(jnp.int32, (days, width), 0) + lax.axis_index(ROWS) * days
    row = lax.broadcasted_iota(jnp.int32, (QUAD, width), 0)
    for w in range(windows):
        live = day >= starts_ref[w : w + 1, :]
        kept = jnp.where(live, returns_ref[w], 0.0)
        number = jnp.sum(live.astype(F32), axis=0, keepdims=True)
        shift = jnp.sum(kept, axis=0, keepdims=True) / jnp.maximum(number, 1.0)
        high = shift.astype(BF16).astype(F32)
        middle = (shift - high).astype(BF16).astype(F32)
        low = (shift - high - middle).astype(BF16).astype(F32)
        shift = high + middle + low
        rest = jnp.where(live, kept - shift, 0.0)
        carried = jnp.where(row == 0, high, jnp.where(row == 1, middle, jnp.where(row == 2, low, 0.0)))
        blocks = [rest[i : i + QUAD] for i in range(0, days, QUAD)] + [carried]
        for i, block in enumerate(blocks):
            block = block.astype(BF16)
            for j in range(parts):
                out_ref[w * parts + j, :, i * LANES : (i + 1) * LANES] = block[:, j * LANES : (j + 1) * LANES]


def scale_kernel(got_ref, starts_ref, block_ref, out_ref):
    sources = got_ref.shape[0]
    days = (got_ref.shape[2] // LANES - 1) * QUAD
    total = sources * days
    parts = sources // starts_ref.shape[0]
    w = lax.axis_index("window")
    own = pl.ds(pl.multiple_of(lax.axis_index(ROWS) % parts * LANES, LANES), LANES)
    starts = starts_ref[:, own]
    starts = jnp.sum(jnp.where(lax.broadcasted_iota(jnp.int32, starts.shape, 0) == w, starts, 0), axis=0, keepdims=True)
    got = got_ref[...].astype(F32)
    lanes = [got[:, :, at : at + LANES] for at in range(0, got.shape[2], LANES)]
    shift = jnp.sum(lanes[-1], axis=1, keepdims=True)
    eights = [jnp.concatenate(lanes[i : i + 2], axis=1) + shift for i in range(0, len(lanes) - 1, 2)]
    values = jnp.concatenate([eight.reshape(sources * EIGHT, LANES) for eight in eights], axis=0)
    row = lax.broadcasted_iota(jnp.int32, (total, LANES), 0)
    eight, source = row // (sources * EIGHT), row % (sources * EIGHT) // EIGHT
    live = source * days + eight * EIGHT + row % EIGHT >= starts
    counts = (total - starts).astype(F32)
    mean = jnp.sum(jnp.where(live, values, 0.0), axis=0, keepdims=True) / counts
    centered = jnp.where(live, values - mean, 0.0)
    squares = jnp.sum(centered * centered, axis=0, keepdims=True)
    scaled = centered * lax.rsqrt(squares + 1.0)
    out_ref[0:total, :] = scaled.astype(BF16)
    out_ref[total:, :] = block_ref[w, :, own].astype(BF16)


def gram_kernel(both_ref, out_ref, all_ref):
    cores, rows, _ = both_ref.shape
    total = rows // LANES * LANES
    both = jnp.concatenate([both_ref[c] for c in range(cores)], axis=1)
    scaled, rounded = both[:total], both[total:]
    blocks = total // LANES
    across = ((1,), (1,))
    proj = dot(rounded, scaled, across, None)
    rest = []
    at = 0

    def put(tile):
        nonlocal at
        all_ref[at : at + tile.shape[0], :] = tile
        at += tile.shape[0]

    for a in range(blocks):
        here, on = slice(a * LANES, (a + 1) * LANES), slice(a * LANES, total)
        strip = dot(scaled[here], scaled[on], across, None)
        put(strip[:HALF, :LANES])
        rest.append(strip[HALF:, :LANES])
        for b in range(1, blocks - a):
            put(strip[:, b * LANES : (b + 1) * LANES])
    left = lax.broadcasted_iota(jnp.int32, (HALF, LANES), 1) < HALF
    for a in range(0, blocks, 2):
        put(jnp.where(left, pltpu.roll(rest[a], HALF, 1), rest[a + 1]))
    for b in range(blocks):
        put(proj[:, b * LANES : (b + 1) * LANES])
    if at < all_ref.shape[0]:
        all_ref[at:, :] = jnp.zeros((all_ref.shape[0] - at, LANES), F32)
    share = out_ref.shape[0]
    out_ref[...] = all_ref[pl.ds(pl.multiple_of(lax.axis_index("sub") * share, EIGHT), share), :]


def inverse_lower(gram):
    k = gram.shape[0]
    size = 8
    row = lax.broadcasted_iota(jnp.int32, (k, LANES), 0)
    lane = lax.broadcasted_iota(jnp.int32, (k, LANES), 1)
    both = jnp.concatenate([gram, jnp.zeros((k, LANES - k), F32)], axis=1)
    both = jnp.where(lane == row + k, 1.0, both)
    for i in range(0, k, size):
        columns = [jnp.broadcast_to(both[:, i + q : i + q + 1], (k, LANES)) for q in range(size)]
        lines = [both[i + q : i + q + 1, :] for q in range(size)]
        inner = {(q, p): columns[q][i + p : i + p + 1, :] for q in range(size) for p in range(q, size)}
        update = jnp.zeros((k, LANES), F32)
        for q in range(size):
            inverse = 1.0 / inner[q, q]
            later = range(q + 1, size)
            ratio = {p: inner[q, p] * inverse for p in later}
            for p in later:
                for r in range(p, size):
                    inner[p, r] -= ratio[p] * inner[q, r]
            for p in later:
                lines[p] -= ratio[p] * lines[q]
                columns[p] -= columns[q] * ratio[p]
            update += jnp.where(row > i + q, columns[q] * inverse, 0.0) * lines[q]
        both -= update
    pivots = jnp.sum(jnp.where(lane == row, both, 0.0), axis=1, keepdims=True)
    return (both * lax.rsqrt(pivots))[:, k : 2 * k]


def iterate_kernel(assets, got_ref, scaled_ref, out_ref, high_ref, low_ref):
    factors = out_ref.shape[1]
    total = scaled_ref.shape[0] - factors
    blocks = total // LANES
    row = lax.broadcasted_iota(jnp.int32, (LANES, LANES), 0)
    lane = lax.broadcasted_iota(jnp.int32, (LANES, LANES), 1)
    at = 0

    def take(rows):
        nonlocal at
        at += rows
        return got_ref[at - rows : at, :]

    tops = []
    for a in range(blocks):
        here = slice(a * LANES, (a + 1) * LANES)
        tops.append(take(HALF))
        for b in range(a + 1, blocks):
            there = slice(b * LANES, (b + 1) * LANES)
            tile = take(LANES)
            high_ref[here, there], low_ref[here, there] = split(tile)
            high_ref[there, here], low_ref[there, here] = split(tile.T)
    for a in range(0, blocks, 2):
        pair = take(HALF)
        for c, rest in ((a, pltpu.roll(pair, HALF, 1)), (a + 1, pair)):
            here = slice(c * LANES, (c + 1) * LANES)
            tile = jnp.concatenate([tops[c], rest], axis=0)
            tile = jnp.where((row >= HALF) & (lane < HALF), tile.T, tile)
            high_ref[here, here], low_ref[here, here] = split(tile)
    proj = jnp.concatenate([take(factors) for b in range(blocks)], axis=1)
    inward = ((1,), (0,))
    for step in range(ITERS):
        high, low = split(proj)
        stacked = dot(jnp.concatenate([high, low], axis=0), high_ref[...], inward, None)
        moved = stacked[:factors] + (stacked[factors:] + dot(high, low_ref[...], inward, None))
        gram = dot(moved, proj, ((1,), (1,))) * (1.0 / assets)
        proj = dot(inverse_lower(gram), moved if step < ITERS - 1 else proj, inward)
    high, low = split(proj)
    scaled = scaled_ref[0:total, :]
    loadings = (dot(high, scaled, inward, None) + dot(low, scaled, inward, None)).astype(BF16)
    out_ref[...] = jnp.broadcast_to(loadings[None], out_ref.shape)


def unpack_kernel(got_ref, out_ref):
    windows, _, width = out_ref.shape
    near, blocks = got_ref.shape[:2]
    for w in range(windows):
        for j in range(width // LANES):
            block = w * (blocks // windows) + j // near
            out_ref[w, :, j * LANES : (j + 1) * LANES] = got_ref[j % near, block].astype(F32)


def on_device(returns, starts, start_block):
    windows, days, width = returns.shape
    factors = start_block.shape[1]
    parts = width // LANES
    rows = windows * parts
    cols, sub = lax.axis_size("cols"), lax.axis_size("sub")
    sides = cols * sub
    total = days * rows
    assets = width * sides
    quad, block = ("mid", "near"), ("cols", "near")

    packed = pl.pallas_call(
        pack_kernel,
        out_shape=jax.ShapeDtypeStruct((rows, QUAD, (days // QUAD + 1) * LANES), BF16),
        in_specs=[VMEM, VMEM],
        out_specs=VMEM,
        name="pack",
    )(returns, starts)
    got = lax.all_to_all(packed, ROWS, 0, 0, tiled=True)

    blocks = total // LANES
    filled = blocks * (blocks - 1) // 2 * LANES + blocks // 2 * 3 * HALF + factors * blocks
    unit = EIGHT * sub * lax.axis_size(block)
    height = (filled + unit - 1) // unit * unit
    scaled = pl.pallas_call(
        scale_kernel,
        out_shape=jax.ShapeDtypeStruct((total + factors, LANES), BF16),
        in_specs=[VMEM, VMEM, VMEM],
        out_specs=VMEM,
        compiler_params=PARAMS,
        name="scale",
    )(got, starts, start_block)
    both = lax.all_gather(scaled, "sub")
    partial = pl.pallas_call(
        gram_kernel,
        out_shape=jax.ShapeDtypeStruct((height // sub, LANES), F32),
        in_specs=[VMEM],
        out_specs=VMEM,
        scratch_shapes=[pltpu.VMEM((height, LANES), F32)],
        compiler_params=PARAMS,
        name="gram",
    )(both)

    pieces = lax.axis_size(block)
    share = height // sub // pieces
    own = lax.all_to_all(partial.reshape(pieces, share, LANES), block, 0, 0, tiled=True).sum(axis=0)
    own = lax.all_gather(own, "mid").sum(axis=0)
    own = lax.all_gather(own, "far").sum(axis=0)
    own = lax.all_to_all(jnp.broadcast_to(own[None], (pieces, share, LANES)), block, 0, 0, tiled=True)
    whole = lax.all_gather(own.reshape(height // sub, LANES), "sub", tiled=True)

    far = windows * parts // NEAR
    sent = pl.pallas_call(
        functools.partial(iterate_kernel, assets),
        out_shape=jax.ShapeDtypeStruct((far, factors, LANES), BF16),
        in_specs=[VMEM, VMEM],
        out_specs=VMEM,
        scratch_shapes=[pltpu.VMEM((total, total), BF16)] * 2,
        compiler_params=PARAMS,
        name="iterate",
    )(whole, scaled)
    got = lax.all_to_all(sent, ("window", "far"), 0, 0, tiled=True)
    got = lax.all_to_all(jnp.broadcast_to(got[None], (NEAR, *got.shape)), quad, 0, 0, tiled=True)
    return pl.pallas_call(
        unpack_kernel,
        out_shape=jax.ShapeDtypeStruct((windows, factors, width), F32),
        in_specs=[VMEM],
        out_specs=VMEM,
        compiler_params=PARAMS,
        name="unpack",
    )(got)


def solution(mesh):
    groups, rows, cols, sub = (mesh.shape[name] for name in ("groups", "rows", "cols", "sub"))

    def whole(returns, starts, start_block):
        windows = returns.shape[0] // groups
        split = Mesh(
            mesh.devices.reshape(groups, windows, rows // windows // NEAR, NEAR // 2, 2, cols, sub),
            ("groups", "window", "far", "mid", "near", "cols", "sub"),
        )
        placed = (
            P("groups", ("window", "far", "mid", "near"), ("cols", "sub")),
            P("groups", ("cols", "sub")),
            P("groups", None, ("cols", "sub")),
        )
        return jax.shard_map(
            on_device,
            mesh=split,
            in_specs=placed,
            out_specs=P("groups", None, ("cols", "sub")),
            check_vma=False,
        )(returns, starts, start_block)

    return whole
```

```python
import functools

import jax
import jax.numpy as jnp
from jax import lax
from jax.experimental import pallas as pl
from jax.experimental.pallas import tpu as pltpu
from jax.sharding import Mesh
from jax.sharding import PartitionSpec as P

ITERS = 3
LANES = 128
ROWS = ("window", "far", "mid", "near")
HALF = LANES // 2
NEAR = 4
EIGHT = 8
QUAD = 4
F32 = jnp.float32
BF16 = jnp.bfloat16
HIGHEST = lax.Precision.HIGHEST
VMEM = pl.BlockSpec(memory_space=pltpu.VMEM)
PARAMS = pltpu.CompilerParams(vmem_limit_bytes=16 << 20)


def dot(a, b, dims, precision=HIGHEST):
    return lax.dot_general(a, b, (dims, ((), ())), precision=precision, preferred_element_type=F32)


def split(a):
    high = a.astype(BF16)
    return high, (a - high.astype(F32)).astype(BF16)


def pack_kernel(returns_ref, starts_ref, out_ref):
    windows, days, width = returns_ref.shape
    parts = width // LANES
    day = lax.broadcasted_iota(jnp.int32, (days, width), 0) + lax.axis_index(ROWS) * days
    row = lax.broadcasted_iota(jnp.int32, (QUAD, width), 0)
    for w in range(windows):
        live = day >= starts_ref[w : w + 1, :]
        kept = jnp.where(live, returns_ref[w], 0.0)
        number = jnp.sum(live.astype(F32), axis=0, keepdims=True)
        shift = jnp.sum(kept, axis=0, keepdims=True) / jnp.maximum(number, 1.0)
        high = shift.astype(BF16).astype(F32)
        middle = (shift - high).astype(BF16).astype(F32)
        low = (shift - high - middle).astype(BF16).astype(F32)
        shift = high + middle + low
        rest = jnp.where(live, kept - shift, 0.0)
        carried = jnp.where(row == 0, high, jnp.where(row == 1, middle, jnp.where(row == 2, low, 0.0)))
        blocks = [rest[i : i + QUAD] for i in range(0, days, QUAD)] + [carried]
        for i, block in enumerate(blocks):
            block = block.astype(BF16)
            for j in range(parts):
                out_ref[w * parts + j, :, i * LANES : (i + 1) * LANES] = block[:, j * LANES : (j + 1) * LANES]


def scale_kernel(got_ref, starts_ref, block_ref, out_ref):
    sources = got_ref.shape[0]
    days = (got_ref.shape[2] // LANES - 1) * QUAD
    total = sources * days
    parts = sources // starts_ref.shape[0]
    w = lax.axis_index("window")
    own = pl.ds(pl.multiple_of(lax.axis_index(ROWS) % parts * LANES, LANES), LANES)
    starts = starts_ref[:, own]
    starts = jnp.sum(jnp.where(lax.broadcasted_iota(jnp.int32, starts.shape, 0) == w, starts, 0), axis=0, keepdims=True)
    got = got_ref[...].astype(F32)
    lanes = [got[:, :, at : at + LANES] for at in range(0, got.shape[2], LANES)]
    shift = jnp.sum(lanes[-1], axis=1, keepdims=True)
    eights = [jnp.concatenate(lanes[i : i + 2], axis=1) + shift for i in range(0, len(lanes) - 1, 2)]
    values = jnp.concatenate([eight.reshape(sources * EIGHT, LANES) for eight in eights], axis=0)
    row = lax.broadcasted_iota(jnp.int32, (total, LANES), 0)
    eight, source = row // (sources * EIGHT), row % (sources * EIGHT) // EIGHT
    live = source * days + eight * EIGHT + row % EIGHT >= starts
    counts = (total - starts).astype(F32)
    mean = jnp.sum(jnp.where(live, values, 0.0), axis=0, keepdims=True) / counts
    centered = jnp.where(live, values - mean, 0.0)
    squares = jnp.sum(centered * centered, axis=0, keepdims=True)
    scaled = centered * lax.rsqrt(squares + 1.0)
    out_ref[0:total, :] = scaled.astype(BF16)
    out_ref[total:, :] = block_ref[w, :, own].astype(BF16)


def gram_kernel(both_ref, out_ref, all_ref):
    cores, rows, _ = both_ref.shape
    total = rows // LANES * LANES
    both = jnp.concatenate([both_ref[c] for c in range(cores)], axis=1)
    scaled, rounded = both[:total], both[total:]
    blocks = total // LANES
    across = ((1,), (1,))
    proj = dot(rounded, scaled, across, None)
    rest = []
    at = 0

    def put(tile):
        nonlocal at
        all_ref[at : at + tile.shape[0], :] = tile
        at += tile.shape[0]

    for a in range(blocks):
        here, on = slice(a * LANES, (a + 1) * LANES), slice(a * LANES, total)
        strip = dot(scaled[here], scaled[on], across, None)
        put(strip[:HALF, :LANES])
        rest.append(strip[HALF:, :LANES])
        for b in range(1, blocks - a):
            put(strip[:, b * LANES : (b + 1) * LANES])
    left = lax.broadcasted_iota(jnp.int32, (HALF, LANES), 1) < HALF
    for a in range(0, blocks, 2):
        put(jnp.where(left, pltpu.roll(rest[a], HALF, 1), rest[a + 1]))
    for b in range(blocks):
        put(proj[:, b * LANES : (b + 1) * LANES])
    if at < all_ref.shape[0]:
        all_ref[at:, :] = jnp.zeros((all_ref.shape[0] - at, LANES), F32)
    share = out_ref.shape[0]
    out_ref[...] = all_ref[pl.ds(pl.multiple_of(lax.axis_index("sub") * share, EIGHT), share), :]


def inverse_lower(gram):
    k = gram.shape[0]
    size = 8
    row = lax.broadcasted_iota(jnp.int32, (k, LANES), 0)
    lane = lax.broadcasted_iota(jnp.int32, (k, LANES), 1)
    both = jnp.concatenate([gram, jnp.zeros((k, LANES - k), F32)], axis=1)
    both = jnp.where(lane == row + k, 1.0, both)
    for i in range(0, k, size):
        columns = [jnp.broadcast_to(both[:, i + q : i + q + 1], (k, LANES)) for q in range(size)]
        lines = [both[i + q : i + q + 1, :] for q in range(size)]
        inner = {(q, p): columns[q][i + p : i + p + 1, :] for q in range(size) for p in range(q, size)}
        update = jnp.zeros((k, LANES), F32)
        for q in range(size):
            inverse = 1.0 / inner[q, q]
            later = range(q + 1, size)
            ratio = {p: inner[q, p] * inverse for p in later}
            for p in later:
                for r in range(p, size):
                    inner[p, r] -= ratio[p] * inner[q, r]
            for p in later:
                lines[p] -= ratio[p] * lines[q]
                columns[p] -= columns[q] * ratio[p]
            update += jnp.where(row > i + q, columns[q] * inverse, 0.0) * lines[q]
        both -= update
    pivots = jnp.sum(jnp.where(lane == row, both, 0.0), axis=1, keepdims=True)
    return (both * lax.rsqrt(pivots))[:, k : 2 * k]


def iterate_kernel(assets, got_ref, scaled_ref, out_ref, high_ref, low_ref):
    factors = out_ref.shape[1]
    total = scaled_ref.shape[0] - factors
    blocks = total // LANES
    row = lax.broadcasted_iota(jnp.int32, (LANES, LANES), 0)
    lane = lax.broadcasted_iota(jnp.int32, (LANES, LANES), 1)
    at = 0

    def take(rows):
        nonlocal at
        at += rows
        return got_ref[at - rows : at, :]

    tops = []
    for a in range(blocks):
        here = slice(a * LANES, (a + 1) * LANES)
        tops.append(take(HALF))
        for b in range(a + 1, blocks):
            there = slice(b * LANES, (b + 1) * LANES)
            tile = take(LANES)
            high_ref[here, there], low_ref[here, there] = split(tile)
            high_ref[there, here], low_ref[there, here] = split(tile.T)
    for a in range(0, blocks, 2):
        pair = take(HALF)
        for c, rest in ((a, pltpu.roll(pair, HALF, 1)), (a + 1, pair)):
            here = slice(c * LANES, (c + 1) * LANES)
            tile = jnp.concatenate([tops[c], rest], axis=0)
            tile = jnp.where((row >= HALF) & (lane < HALF), tile.T, tile)
            high_ref[here, here], low_ref[here, here] = split(tile)
    proj = jnp.concatenate([take(factors) for b in range(blocks)], axis=1)
    inward = ((1,), (0,))
    for step in range(ITERS):
        high, low = split(proj)
        stacked = dot(jnp.concatenate([high, low], axis=0), high_ref[...], inward, None)
        moved = stacked[:factors] + (stacked[factors:] + dot(high, low_ref[...], inward, None))
        gram = dot(moved, proj, ((1,), (1,))) * (1.0 / assets)
        proj = dot(inverse_lower(gram), moved if step < ITERS - 1 else proj, inward)
    high, low = split(proj)
    scaled = scaled_ref[0:total, :]
    loadings = (dot(high, scaled, inward, None) + dot(low, scaled, inward, None)).astype(BF16)
    out_ref[...] = jnp.broadcast_to(loadings[None], out_ref.shape)


def unpack_kernel(got_ref, out_ref):
    windows, _, width = out_ref.shape
    near = got_ref.shape[0]
    for w in range(windows):
        for j in range(width // LANES):
            block = j // near * windows + w
            out_ref[w, :, j * LANES : (j + 1) * LANES] = got_ref[j % near, block].astype(F32)


def on_device(returns, starts, start_block):
    windows, days, width = returns.shape
    factors = start_block.shape[1]
    parts = width // LANES
    rows = windows * parts
    cols, sub = lax.axis_size("cols"), lax.axis_size("sub")
    sides = cols * sub
    total = days * rows
    assets = width * sides
    quad, block = ("mid", "near"), ("cols", "near")

    packed = pl.pallas_call(
        pack_kernel,
        out_shape=jax.ShapeDtypeStruct((rows, QUAD, (days // QUAD + 1) * LANES), BF16),
        in_specs=[VMEM, VMEM],
        out_specs=VMEM,
        name="pack",
    )(returns, starts)
    got = lax.all_to_all(packed, ROWS, 0, 0, tiled=True)

    blocks = total // LANES
    filled = blocks * (blocks - 1) // 2 * LANES + blocks // 2 * 3 * HALF + factors * blocks
    unit = EIGHT * sub * lax.axis_size(block)
    height = (filled + unit - 1) // unit * unit
    scaled = pl.pallas_call(
        scale_kernel,
        out_shape=jax.ShapeDtypeStruct((total + factors, LANES), BF16),
        in_specs=[VMEM, VMEM, VMEM],
        out_specs=VMEM,
        compiler_params=PARAMS,
        name="scale",
    )(got, starts, start_block)
    both = lax.all_gather(scaled, "sub")
    partial = pl.pallas_call(
        gram_kernel,
        out_shape=jax.ShapeDtypeStruct((height // sub, LANES), F32),
        in_specs=[VMEM],
        out_specs=VMEM,
        scratch_shapes=[pltpu.VMEM((height, LANES), F32)],
        compiler_params=PARAMS,
        name="gram",
    )(both)

    pieces = lax.axis_size(block)
    share = height // sub // pieces
    own = lax.all_to_all(partial.reshape(pieces, share, LANES), block, 0, 0, tiled=True).sum(axis=0)
    own = lax.all_gather(own, "mid").sum(axis=0)
    own = lax.all_gather(own, "far").sum(axis=0)
    own = lax.all_to_all(jnp.broadcast_to(own[None], (pieces, share, LANES)), block, 0, 0, tiled=True)
    whole = lax.all_gather(own.reshape(height // sub, LANES), "sub", tiled=True)

    far = windows * parts // NEAR
    sent = pl.pallas_call(
        functools.partial(iterate_kernel, assets),
        out_shape=jax.ShapeDtypeStruct((far, factors, LANES), BF16),
        in_specs=[VMEM, VMEM],
        out_specs=VMEM,
        scratch_shapes=[pltpu.VMEM((total, total), BF16)] * 2,
        compiler_params=PARAMS,
        name="iterate",
    )(whole, scaled)
    got = lax.all_to_all(sent, ("far", "window"), 0, 0, tiled=True)
    got = lax.all_to_all(jnp.broadcast_to(got[None], (NEAR, *got.shape)), quad, 0, 0, tiled=True)
    return pl.pallas_call(
        unpack_kernel,
        out_shape=jax.ShapeDtypeStruct((windows, factors, width), F32),
        in_specs=[VMEM],
        out_specs=VMEM,
        compiler_params=PARAMS,
        name="unpack",
    )(got)


def solution(mesh):
    groups, rows, cols, sub = (mesh.shape[name] for name in ("groups", "rows", "cols", "sub"))

    def whole(returns, starts, start_block):
        windows = returns.shape[0] // groups
        split = Mesh(
            mesh.devices.reshape(groups, windows, rows // windows // NEAR, NEAR // 2, 2, cols, sub),
            ("groups", "window", "far", "mid", "near", "cols", "sub"),
        )
        placed = (
            P("groups", ("window", "far", "mid", "near"), ("cols", "sub")),
            P("groups", ("cols", "sub")),
            P("groups", None, ("cols", "sub")),
        )
        return jax.shard_map(
            on_device,
            mesh=split,
            in_specs=placed,
            out_specs=P("groups", None, ("cols", "sub")),
            check_vma=False,
        )(returns, starts, start_block)

    return whole
```
